512 devices in a mesh: dp: 16 (over z_hi, y, core), expert: 32 (over x, z_lo).
Axes of the slice: x: 4, y: 4, z: 16 (z_hi: 2, z_lo: 8; z = z_hi * 8 + z_lo), core: 2. Of those that a mesh axis runs over, the one named last changes fastest.
Arguments:
- tokens: bfloat16 [65536, 1024], P(('dp', 'expert')), may hold values from -6 to 6
- chosen_expert_index: int32 [65536, 6], P(('dp', 'expert')), may hold values from 0 to 31, as said below
- router_gate_weight: float32 [65536, 6], P(('dp', 'expert')), may hold values from 0.05 to 0.5
- output_gradient: bfloat16 [65536, 1024], P(('dp', 'expert')), may hold values from -0.15917969 to 0.15917969
- gate_weight_matrix: bfloat16 [32, 1024, 704], P('expert'), may hold values from -0.1875 to 0.1875
- up_weight: bfloat16 [32, 1024, 704], P('expert'), may hold values from -0.1875 to 0.1875
- down_weight: bfloat16 [32, 704, 1024], P('expert'), may hold values from -0.21875 to 0.21875
- adapter_down_maps: bfloat16 [32, 16, 704], P('expert'), may hold values from -0.21875 to 0.21875
- adapter_up_maps: bfloat16 [32, 16, 1024], P('expert'), may hold values from -1.5 to 1.5
Outputs:
- mixed: bfloat16 [65536, 1024], P(('dp', 'expert'))
- grad_in: bfloat16 [32, 16, 704], P('expert')
- grad_out: bfloat16 [32, 16, 1024], P('expert')
The draws below stay inside these ranges and needn't reach their ends.
Inputs may be any that keep to these rules, and one draw needn't show every extreme that they name: `chosen_expert_index`: each row names 6 different experts. In each aligned block of 128 rows (the rows of one device) no expert is named by more than 48 rows, and one and the same expert, drawn for the whole array, is named by exactly 48 rows of every block. Each row's experts are 6 neighbours in one circular order of all experts, drawn for the whole array.
All inputs are finite; a program needn't handle non-finite values.
Results may differ from the reference program's by a relative error of at most 0.0064.
Values may be sent and summed in bfloat16 or wider, within the bound.
A program may use at most 64 MiB of HBM per device.

```python
import math
import jax
import jax.numpy as jnp
from jax import lax

MODEL_FEATURES = 1024
HIDDEN_UNITS = 704
ADAPTER_DEPTH = 16
TOPK = 6
TOK_DEV = 128
ROUTED_EXPERTS = 32
TOKENS = 65536
HOT = 8
CAP = 48


def draw_chosen_expert_index(key, part):
    blocks = TOKENS // TOK_DEV
    others = ROUTED_EXPERTS - TOPK
    order_key, spread_keys = jax.random.split(jax.random.fold_in(key, 11))
    labels = jax.random.permutation(order_key, ROUTED_EXPERTS).astype(jnp.int32)
    position = jnp.arange(TOK_DEV, dtype=jnp.int32)
    offsets = jnp.arange(TOPK, dtype=jnp.int32)

    def one_block(block_key):
        shuffle_key, spread_key = jax.random.split(block_key)
        spread = TOPK + jax.random.permutation(spread_key, others).astype(jnp.int32)
        hot_start = position // HOT
        cold_index = jnp.maximum(position - TOPK * HOT, 0) % others
        cold_start = spread[cold_index]
        start_label = jnp.where(position < TOPK * HOT, hot_start, cold_start).astype(jnp.int32)
        start_label = jax.random.permutation(shuffle_key, start_label)
        return labels[(start_label[:, None] + offsets[None, :]) % ROUTED_EXPERTS]
    block_keys = jax.random.split(spread_keys, blocks)
    return jax.vmap(one_block)(block_keys).reshape(TOKENS, TOPK).astype(jnp.int32)


def levels(own_key, dims, cuts, smallest, high):
    def one(axis_at, parts):
        steps = jax.random.uniform(jax.random.fold_in(jax.random.fold_in(own_key, 6), axis_at), (parts,), jnp.float32, smallest / len(cuts), high / len(cuts))
        return jnp.repeat(jnp.exp(steps), dims[axis_at] // parts).reshape((-1,) + (1,) * (len(dims) - axis_at - 1))

    gain = one(*cuts[0])
    for cut in cuts[1:]:
        gain = gain * one(*cut)
    return gain


def scatter_about(own_key, shape, width, bound, cuts=(), held_as=jnp.bfloat16):
    values = width * jax.random.normal(own_key, shape, jnp.float32)
    if cuts:
        values = values * levels(own_key, shape, cuts, -0.22, 0.18)
    return jnp.clip(values, -bound, bound).astype(held_as)


def setup_inputs(seed: int = 0) -> dict:
    seeds = jax.random.split(jax.random.key(seed), 10)
    return {
        "tokens": scatter_about(seeds[0], (TOKENS, MODEL_FEATURES), 1.0, 6.0, ((0, 512),)),
        "chosen_expert_index": draw_chosen_expert_index(jax.random.fold_in(seeds[9], 71), 0),
        "router_gate_weight": jnp.clip(jnp.exp(math.log(0.5) - 2.3025851 * jax.random.uniform(seeds[2], (TOKENS, TOPK), jnp.float32) ** levels(seeds[2], (TOKENS, TOPK), ((0, 512),), -0.2, 0.2)), 0.05, 0.5),
        "output_gradient": scatter_about(seeds[3], (TOKENS, MODEL_FEATURES), 0.02, 0.15917969, ((0, 512),)),
        "gate_weight_matrix": scatter_about(seeds[4], (ROUTED_EXPERTS, MODEL_FEATURES, HIDDEN_UNITS), MODEL_FEATURES ** -0.5, 0.1875, ((0, 32),)),
        "up_weight": scatter_about(seeds[5], (ROUTED_EXPERTS, MODEL_FEATURES, HIDDEN_UNITS), MODEL_FEATURES ** -0.5, 0.1875, ((0, 32),)),
        "down_weight": scatter_about(seeds[6], (ROUTED_EXPERTS, HIDDEN_UNITS, MODEL_FEATURES), HIDDEN_UNITS ** -0.5, 0.21875, ((0, 32),)),
        "adapter_down_maps": scatter_about(seeds[7], (ROUTED_EXPERTS, ADAPTER_DEPTH, HIDDEN_UNITS), HIDDEN_UNITS ** -0.5, 0.21875, ((0, 32),)),
        "adapter_up_maps": scatter_about(seeds[8], (ROUTED_EXPERTS, ADAPTER_DEPTH, MODEL_FEATURES), ADAPTER_DEPTH ** -0.5, 1.5, ((0, 32),)),
    }


def reference(tokens, chosen_expert_index, router_gate_weight, output_gradient, gate_weight_matrix, up_weight, down_weight, adapter_down_maps, adapter_up_maps):
    total_slots = TOKENS * TOPK
    flat_ids = chosen_expert_index.reshape(total_slots).astype(jnp.int32)
    flat_gates = router_gate_weight.reshape(total_slots)
    sort_order = jnp.argsort(flat_ids, stable=True).astype(jnp.int32)
    counts = jnp.bincount(flat_ids, length=ROUTED_EXPERTS).astype(jnp.int32)
    starts = (jnp.cumsum(counts) - counts).astype(jnp.int32)
    bound_rows = (TOKENS // TOK_DEV) * CAP

    def per_expert(running, expert_number):
        position = jnp.arange(bound_rows, dtype=jnp.int32)
        is_live = position < counts[expert_number]
        slot_index = sort_order[jnp.clip(starts[expert_number] + position, 0, total_slots - 1).astype(jnp.int32)]
        token_index = (slot_index // TOPK).astype(jnp.int32)
        slot_gate = jnp.where(is_live, flat_gates[slot_index], jnp.float32(0.0))
        slot_rows = tokens[token_index]
        gate_proj = jnp.dot(slot_rows, gate_weight_matrix[expert_number], preferred_element_type=jnp.float32)
        upward = jnp.dot(slot_rows, up_weight[expert_number], preferred_element_type=jnp.float32)
        hidden_state = (jax.nn.silu(gate_proj) * upward).astype(jnp.bfloat16)
        rank_state = jnp.dot(hidden_state, adapter_down_maps[expert_number].T, preferred_element_type=jnp.float32).astype(jnp.bfloat16)
        slot_out = (jnp.dot(hidden_state, down_weight[expert_number], preferred_element_type=jnp.float32)
                    + jnp.dot(rank_state, adapter_up_maps[expert_number], preferred_element_type=jnp.float32)).astype(jnp.bfloat16)
        running = running.at[token_index].add(slot_gate[:, None] * slot_out.astype(jnp.float32))
        expert_slot_gradient = (slot_gate[:, None] * output_gradient[token_index].astype(jnp.float32)).astype(jnp.bfloat16)
        rank_gradient = jnp.dot(expert_slot_gradient, adapter_up_maps[expert_number].T, preferred_element_type=jnp.float32).astype(jnp.bfloat16)
        grad_hidden = jnp.dot(rank_gradient.T, hidden_state, preferred_element_type=jnp.float32)
        grad_model = jnp.dot(rank_state.T, expert_slot_gradient, preferred_element_type=jnp.float32)
        return running, (grad_hidden, grad_model)

    initial = jnp.zeros((TOKENS, MODEL_FEATURES), jnp.float32)
    mixed_sum, grads = lax.scan(per_expert, initial, jnp.arange(ROUTED_EXPERTS, dtype=jnp.int32))
    return mixed_sum.astype(jnp.bfloat16), grads[0].astype(jnp.bfloat16), grads[1].astype(jnp.bfloat16)
```

```python
import functools

import jax
import jax.numpy as jnp
from jax import lax
from jax.experimental import pallas as pl
from jax.experimental.pallas import tpu as pltpu
from jax.sharding import PartitionSpec as P

BF = jnp.bfloat16
F32 = jnp.float32
XS, ZL, ZS, YS = 4, 8, 16, 4
CAP = 48
ROWS = XS * CAP
VOID = -1000.0


def mm(a, b):
    return jnp.dot(a, b, preferred_element_type=F32)


def mm_nt(a, b):
    return lax.dot_general(a, b, (((1,), (1,)), ((), ())), preferred_element_type=F32)


def kernel(
    m_ref, tok_hbm, dy_hbm, wg_hbm, wu_hbm, wd_hbm, ad_hbm, au_hbm,
    mixed_ref, gin_ref, gout_ref,
    tbuf, dbuf, mbuf, abuf, wg, wu, wd, ad,
    ssend, srecv, hbuf, osend, oret, lgs, lgr, lrs, lrr, rss, rsr,
    gi, go, gor, dpa, dpr, dpb, dpq, dpo, dpf,
    ld_sem, t_s, t_r, m_s, m_r, d_s, d_r, a_s, a_r, x_s, x_r, lg_s, lg_r,
    o_s, o_r, lr_s, lr_r, r_s, r_r, go_s, go_r, da_s, da_r, db_s, db_r, dc_s, dc_r,
):
    depth = ad_hbm.shape[1]
    hidden = wg_hbm.shape[2]
    toks = tok_hbm.shape[0]
    half = toks // 2
    d = lax.axis_index("dp")
    e = lax.axis_index("expert")
    core = lax.rem(d, 2)
    y = lax.rem(lax.div(d, 2), YS)
    zh = lax.div(d, 2 * YS)
    x = lax.div(e, ZL)
    zl = lax.rem(e, ZL)
    z = zh * ZL + zl
    way = 1 - 2 * core
    k = y * 2 + core

    def at(x_, z_):
        return {"dp": lax.div(z_, ZL) * (2 * YS) + k, "expert": x_ * ZL + lax.rem(z_, ZL)}

    def ring(step):
        return lax.rem(z + step + ZS, ZS)

    def xq(q):
        return lax.rem(x + q + XS, XS)

    def peer(r):
        kk = lax.rem(k + r, 2 * YS)
        return kk, {"dp": zh * (2 * YS) + kk, "expert": e}

    def remote(src, dst, s, r, dev):
        return pltpu.make_async_remote_copy(
            src_ref=src, dst_ref=dst, send_sem=s, recv_sem=r,
            device_id=dev, device_id_type=pl.DeviceIdType.MESH)

    def out_step(i):
        return way * (2 * lax.rem(i, 2) - 1)

    def tok_copy(i, h):
        src = jnp.maximum(i - 2, 0)
        rows = pl.ds(h * half, half)
        return remote(tbuf.at[src, rows], tbuf.at[i, rows], t_s.at[i, h], t_r.at[i, h],
                      at(x, ring(out_step(i))))

    def dy_copy(i):
        src = jnp.maximum(i - 2, 0)
        return remote(dbuf.at[src], dbuf.at[i], d_s.at[i], d_r.at[i], at(x, ring(out_step(i))))

    def m_copy(i):
        zt = ring(out_step(i) * ((i + 1) // 2))
        return remote(m_ref.at[lax.rem(zt, ZL)], mbuf.at[i], m_s.at[i], m_r.at[i], at(x, zt))

    def a_copy(q):
        return remote(abuf.at[pl.ds(0, depth)], abuf.at[pl.ds(q * depth, depth)],
                      a_s.at[q], a_r.at[q], at(xq(-q), z))

    def x_copy(i, q):
        rows = pl.ds(q * CAP, CAP)
        return remote(ssend.at[i, rows], srecv.at[i, rows], x_s.at[i, q], x_r.at[i, q], at(xq(q), z))

    def lg_copy(i, q):
        rows = pl.ds(q * depth, depth)
        return remote(lgs.at[i, rows], lgr.at[i, rows], lg_s.at[i, q], lg_r.at[i, q], at(xq(q), z))

    def o_copy(i, q):
        rows = pl.ds(q * CAP, CAP)
        return remote(osend.at[i, rows], oret.at[i, rows], o_s.at[i, q], o_r.at[i, q], at(xq(-q), z))

    def lr_copy(i, q):
        rows = pl.ds(q * depth, depth)
        return remote(lrs.at[i, rows], lrr.at[i, rows], lr_s.at[i, q], lr_r.at[i, q], at(xq(-q), z))

    def rs_copy(i):
        return remote(rss.at[i], rsr.at[i], r_s.at[i], r_r.at[i], at(x, ring(-out_step(i))))

    def go_copy(q):
        return remote(go.at[pl.ds(q * depth, depth)], gor.at[pl.ds(q * depth, depth)],
                      go_s.at[q], go_r.at[q], at(xq(q), z))

    def da_copy(r):
        kk, dev = peer(r)
        return remote(dpa.at[kk], dpr.at[r], da_s.at[r], da_r.at[r], dev)

    def db_copy():
        return remote(dpb, dpq, db_s, db_r, at(x, ring(ZL)))

    def dc_copy(r):
        _, dev = peer(r)
        return remote(dpo, dpf.at[r], dc_s.at[r], dc_r.at[r], dev)

    loads = [
        pltpu.make_async_copy(tok_hbm, tbuf.at[0], ld_sem.at[0]),
        pltpu.make_async_copy(au_hbm.at[0], abuf.at[pl.ds(0, depth)], ld_sem.at[1]),
        pltpu.make_async_copy(wg_hbm.at[0], wg, ld_sem.at[2]),
        pltpu.make_async_copy(wu_hbm.at[0], wu, ld_sem.at[3]),
        pltpu.make_async_copy(wd_hbm.at[0], wd, ld_sem.at[4]),
        pltpu.make_async_copy(ad_hbm.at[0], ad, ld_sem.at[5]),
        pltpu.make_async_copy(dy_hbm, dbuf.at[0], ld_sem.at[6]),
    ]
    for load in loads:
        load.start()

    barrier = pltpu.get_barrier_semaphore()
    friends = [at(x, ring(s)) for s in (1, -1, 2, -2, 3, -3, 4, -4, ZL)]
    friends += [at(xq(q), z) for q in range(1, XS)]
    friends += [peer(r)[1] for r in range(1, 2 * YS)]
    for friend in friends:
        pl.semaphore_signal(barrier, inc=1, device_id=friend, device_id_type=pl.DeviceIdType.MESH)
    gi[...] = jnp.zeros_like(gi)
    go[...] = jnp.zeros_like(go)
    mbuf[0] = m_ref[zl]
    loads[0].wait()
    loads[1].wait()
    pl.semaphore_wait(barrier, len(friends))

    for i in (1, 2):
        for h in (0, 1):
            tok_copy(i, h).start()
    for i in range(1, 8):
        m_copy(i).start()
    for q in range(1, XS):
        a_copy(q).start()

    row_id = lax.broadcasted_iota(jnp.int32, (CAP, toks), 0).astype(F32)
    row_all = lax.broadcasted_iota(jnp.int32, (toks, toks), 0).astype(F32)
    lane_id = lax.broadcasted_iota(jnp.int32, (toks, ROWS), 1).astype(F32)

    def compact(i):
        m = mbuf[i]
        hot = jnp.concatenate(
            [(row_id == m[XS + q:XS + q + 1]).astype(F32) for q in range(XS)], axis=0).astype(BF)
        rows = mm(hot, tbuf[i]).astype(BF)
        srecv[i, 0:CAP] = rows[0:CAP]
        ssend[i, CAP:ROWS] = rows[CAP:ROWS]
        for q in range(1, XS):
            x_copy(i, q).start()

    def expert(i):
        for q in range(1, XS):
            x_copy(i, q).wait_recv()
        rows = srecv[i]
        g = mm(rows, wg[...])
        u = mm(rows, wu[...])
        h = (g / (1.0 + jnp.exp(-g)) * u).astype(BF)
        hbuf[i] = h
        adm = ad[...]
        low = mm_nt(h, adm).astype(BF)
        for q in range(XS):
            t = mm_nt(adm, h[q * CAP:(q + 1) * CAP]).astype(BF)
            if q == 0:
                lrr[i, 0:depth, 0:CAP] = t
            else:
                lrs[i, q * depth:(q + 1) * depth, 0:CAP] = t
        out = (mm(h, wd[...]) + mm(low, abuf[0:depth])).astype(BF)
        oret[i, 0:CAP] = out[0:CAP]
        osend[i, CAP:ROWS] = out[CAP:ROWS]
        for q in range(1, XS):
            lr_copy(i, q).start()

    compact(0)
    for load in loads[2:]:
        load.wait()

    def inbound(i, c):
        for h in (0, 1):
            tok_copy(i, h).wait_recv()

        @pl.when(i <= 5)
        def _():
            for h in (0, 1):
                tok_copy(i + 2, h).start()

        @pl.when(i == 6)
        def _():
            dy_copy(1).start()
            dy_copy(2).start()

        m_copy_wait(i)
        compact(i)
        expert(i - 1)
        return c

    def m_copy_wait(i):
        remote(m_ref.at[0], mbuf.at[i], m_s.at[i], m_r.at[i], at(x, z)).wait_recv()

    lax.fori_loop(1, 8, inbound, 0)
    for q in range(1, XS):
        a_copy(q).wait_recv()
    for q in range(1, XS):
        o_copy(6, q).start()
    expert(7)
    for q in range(1, XS):
        o_copy(7, q).start()

    def grad_in(n):
        for q in range(1, XS):
            lg_copy(n, q).wait_recv()
        acc = gi[:, 0:hidden]
        for q in range(XS):
            acc += mm(lgr[n, q * depth:(q + 1) * depth, 0:CAP], hbuf[n, q * CAP:(q + 1) * CAP])
        gi[:, 0:hidden] = acc

    def outbound(n, c):
        i = 7 - n

        @pl.when(i >= 2)
        def _():
            for q in range(1, XS):
                o_copy(i - 2, q).start()

        for q in range(1, XS):
            o_copy(i, q).wait_recv()
        mt = mbuf[i].T
        wt = jnp.zeros((toks, ROWS), F32)
        for q in range(XS):
            wt = jnp.where(lane_id == mt[:, XS + q:XS + q + 1] + float(q * CAP), mt[:, q:q + 1], wt)
        hi = wt.astype(BF)
        lo = (wt - hi.astype(F32)).astype(BF)
        rows = oret[i]
        part = mm(hi, rows) + mm(lo, rows)

        @pl.when(i >= 6)
        def _():
            rss[i] = part.astype(BF)

        @pl.when((i >= 1) & (i < 6))
        def _():
            rs_copy(i + 2).wait_recv()
            rss[i] = (part + rsr[i + 2].astype(F32)).astype(BF)

        @pl.when(i >= 1)
        def _():
            rs_copy(i).start()

        @pl.when(i == 0)
        def _():
            rs_copy(1).wait_recv()
            rs_copy(2).wait_recv()
            mixed_ref[...] = (part + rsr[1].astype(F32) + rsr[2].astype(F32)).astype(BF)

        @pl.when(n >= 1)
        def _():
            dy_copy(n).wait_recv()

        @pl.when((n >= 1) & (n <= 5))
        def _():
            dy_copy(n + 2).start()

        m = mbuf[n]
        dy = dbuf[n]
        base = mm_nt(abuf[...], dy)
        lows = []
        for q in range(XS):
            gate = m[q:q + 1]
            rank = m[XS + q:XS + q + 1]
            lg = (base[q * depth:(q + 1) * depth] * gate).astype(BF)
            hot = (row_all == rank).astype(F32).astype(BF)
            packed = mm_nt(lg, hot).astype(BF)
            if q == 0:
                lgr[n, 0:depth] = packed
            else:
                lgs[n, q * depth:(q + 1) * depth] = packed
                lg_copy(n, q).start()
                lr_copy(n, q).wait_recv()
            low = mm(lrr[n, q * depth:(q + 1) * depth, 0:CAP], hot[0:CAP])
            lows.append((low * gate).astype(BF))
        go[...] += mm(jnp.concatenate(lows, axis=0), dy)

        @pl.when(n >= 1)
        def _():
            grad_in(n - 1)

        return c

    lax.fori_loop(0, 8, outbound, 0)

    for q in range(1, XS):
        go_copy(q).start()
    grad_in(7)
    total = go[0:depth]
    for q in range(1, XS):
        go_copy(q).wait_recv()
        total += gor[q * depth:(q + 1) * depth]
    for j in range(2 * YS):
        cols = slice(j * 128, (j + 1) * 128)
        dpa[j, 0:depth] = total[:, cols]
        if j * 128 < hidden:
            dpa[j, depth:2 * depth] = gi[:, cols]
        else:
            dpa[j, depth:2 * depth] = jnp.zeros((depth, 128), F32)
    for r in range(1, 2 * YS):
        da_copy(r).start()
    own = dpa[k]
    for r in range(1, 2 * YS):
        da_copy(r).wait_recv()
        own += dpr[r]
    dpb[...] = own
    db_copy().start()
    db_copy().wait_recv()
    fin = (dpb[...] + dpq[...]).astype(BF)
    dpo[...] = fin
    dpf[0] = fin
    for r in range(1, 2 * YS):
        dc_copy(r).start()
    for r in range(1, 2 * YS):
        dc_copy(r).wait_recv()
    for j in range(2 * YS):
        piece = dpf[lax.rem(k - j + 2 * YS, 2 * YS)]
        gout_ref[:, j * 128:(j + 1) * 128] = piece[0:depth]
        width = min(128, hidden - j * 128)
        if width > 0:
            gin_ref[:, j * 128:j * 128 + width] = piece[depth:2 * depth, 0:width]

    def drain(i, c):
        for q in range(1, XS):
            x_copy(i, q).wait_send()
            lg_copy(i, q).wait_send()
            o_copy(i, q).wait_send()
            lr_copy(i, q).wait_send()

        @pl.when(i >= 1)
        def _():
            for h in (0, 1):
                tok_copy(i, h).wait_send()
            dy_copy(i).wait_send()
            remote(m_ref.at[0], mbuf.at[i], m_s.at[i], m_r.at[i], at(x, z)).wait_send()
            rs_copy(i).wait_send()
            da_copy(i).wait_send()
            dc_copy(i).wait_send()

        return c

    lax.fori_loop(0, 8, drain, 0)
    db_copy().wait_send()
    for q in range(1, XS):
        a_copy(q).wait_send()
        go_copy(q).wait_send()


def shards(tokens, ids, gates, dy, wg, wu, wd, ad, au):
    toks, width = tokens.shape
    depth, hidden = ad.shape[1], ad.shape[2]
    x = lax.axis_index("expert") // ZL
    table = ((x + jnp.arange(XS)[None, :]) % XS) * ZL + jnp.arange(ZL)[:, None]
    hit = ids.T[:, None, None, :] == table.astype(jnp.int32)[None, :, :, None]
    gate = jnp.sum(jnp.where(hit, gates.T[:, None, None, :], 0.0), axis=0)
    chosen = jnp.any(hit, axis=0)
    before = jnp.arange(toks)[:, None] < jnp.arange(toks)[None, :]
    rank = jnp.dot(chosen.astype(BF).reshape(XS * ZL, toks), before.astype(BF),
                   preferred_element_type=F32).reshape(ZL, XS, toks)
    m = jnp.concatenate([gate, jnp.where(chosen, rank, VOID)], axis=1)
    anyspace = pl.BlockSpec(memory_space=pl.ANY)
    vmem = pl.BlockSpec(memory_space=pltpu.VMEM)
    dma = pltpu.SemaphoreType.DMA
    V = pltpu.VMEM
    mixed, gin, gout = pl.pallas_call(
        kernel,
        name="moe",
        out_shape=(
            jax.ShapeDtypeStruct((toks, width), BF),
            jax.ShapeDtypeStruct((depth, hidden), BF),
            jax.ShapeDtypeStruct((depth, width), BF),
        ),
        in_specs=[vmem] + [anyspace] * 7,
        out_specs=(vmem, vmem, vmem),
        scratch_shapes=[
            V((8, toks, width), BF), V((8, toks, width), BF), V((8, 2 * XS, toks), F32),
            V((XS * depth, width), BF),
            V((width, hidden), BF), V((width, hidden), BF), V((hidden, width), BF), V((depth, hidden), BF),
            V((8, ROWS, width), BF), V((8, ROWS, width), BF), V((8, ROWS, hidden), BF),
            V((8, ROWS, width), BF), V((8, ROWS, width), BF),
            V((8, XS * depth, 128), BF), V((8, XS * depth, 128), BF),
            V((8, XS * depth, 128), BF), V((8, XS * depth, 128), BF),
            V((8, toks, width), BF), V((8, toks, width), BF),
            V((depth, 768), F32), V((XS * depth, width), F32), V((XS * depth, width), F32),
            V((8, 2 * depth, 128), F32), V((8, 2 * depth, 128), F32),
            V((2 * depth, 128), F32), V((2 * depth, 128), F32), V((2 * depth, 128), BF),
            V((8, 2 * depth, 128), BF),
            dma((7,)), dma((8, 2)), dma((8, 2)), dma((8,)), dma((8,)), dma((8,)), dma((8,)),
            dma((4,)), dma((4,)), dma((8, 4)), dma((8, 4)), dma((8, 4)), dma((8, 4)),
            dma((8, 4)), dma((8, 4)), dma((8, 4)), dma((8, 4)), dma((8,)), dma((8,)),
            dma((4,)), dma((4,)), dma((8,)), dma((8,)), dma(()), dma(()), dma((8,)), dma((8,)),
        ],
        compiler_params=pltpu.CompilerParams(
            collective_id=0, has_side_effects=True, vmem_limit_bytes=60 * 1024 * 1024),
    )(m, tokens, dy, wg, wu, wd, ad, au)
    return mixed, gin[None], gout[None]


def solution(mesh):
    tok = P(("dp", "expert"), None)
    exp = P("expert", None, None)
    return jax.shard_map(
        shards,
        mesh=mesh,
        in_specs=(tok, tok, tok, tok, exp, exp, exp, exp, exp),
        out_specs=(tok, exp, exp),
        check_vma=False,
    )
```

```python
import functools

import jax
import jax.numpy as jnp
from jax import lax
from jax.experimental import pallas as pl
from jax.experimental.pallas import tpu as pltpu
from jax.sharding import PartitionSpec as P

BF = jnp.bfloat16
F32 = jnp.float32
XS, ZL, ZS, YS = 4, 8, 16, 4
CAP = 48
ROWS = XS * CAP
VOID = -1000.0


def mm(a, b):
    return jnp.dot(a, b, preferred_element_type=F32)


def mm_nt(a, b):
    return lax.dot_general(a, b, (((1,), (1,)), ((), ())), preferred_element_type=F32)


def kernel(
    ids_ref, gates_ref, tok_hbm, dy_hbm, wg_hbm, wu_hbm, wd_hbm, ad_hbm, au_hbm,
    mixed_ref, gin_ref, gout_ref,
    tbuf, dbuf, m_ref, mbuf, abuf, wg, wu, wd, ad,
    ssend, srecv, hbuf, osend, oret, lgs, lgr, lrs, lrr, rss, rsr,
    gi, go, gor, dpa, dpr, dpb, dpq, dpo, dpf,
    ld_sem, t_s, t_r, m_s, m_r, d_s, d_r, a_s, a_r, x_s, x_r, lg_s, lg_r,
    o_s, o_r, lr_s, lr_r, r_s, r_r, go_s, go_r, da_s, da_r, db_s, db_r, dc_s, dc_r, far,
):
    depth = ad_hbm.shape[1]
    hidden = wg_hbm.shape[1]
    choices = ids_ref.shape[0]
    toks = tok_hbm.shape[0]
    half = toks // 2
    d = lax.axis_index("dp")
    e = lax.axis_index("expert")
    core = lax.rem(d, 2)
    y = lax.rem(lax.div(d, 2), YS)
    zh = lax.div(d, 2 * YS)
    x = lax.div(e, ZL)
    zl = lax.rem(e, ZL)
    z = zh * ZL + zl
    way = 1 - 2 * core
    k = y * 2 + core

    def at(x_, z_):
        return {"dp": lax.div(z_, ZL) * (2 * YS) + k, "expert": x_ * ZL + lax.rem(z_, ZL)}

    def ring(step):
        return lax.rem(z + step + ZS, ZS)

    def xq(q):
        return lax.rem(x + q + XS, XS)

    def peer(r):
        kk = lax.rem(k + r, 2 * YS)
        return kk, {"dp": zh * (2 * YS) + kk, "expert": e}

    def remote(src, dst, s, r, dev):
        return pltpu.make_async_remote_copy(
            src_ref=src, dst_ref=dst, send_sem=s, recv_sem=r,
            device_id=dev, device_id_type=pl.DeviceIdType.MESH)

    def out_step(i):
        return way * (2 * lax.rem(i, 2) - 1)

    def tok_copy(i, h):
        src = jnp.maximum(i - 2, 0)
        rows = pl.ds(h * half, half)
        return remote(tbuf.at[src, rows], tbuf.at[i, rows], t_s.at[i, h], t_r.at[i, h],
                      at(x, ring(out_step(i))))

    def dy_copy(i):
        src = jnp.maximum(i - 2, 0)
        return remote(dbuf.at[src], dbuf.at[i], d_s.at[i], d_r.at[i], at(x, ring(out_step(i))))

    def m_copy(i):
        zt = ring(out_step(i) * ((i + 1) // 2))
        return remote(m_ref.at[lax.rem(zt, ZL)], mbuf.at[i], m_s.at[i], m_r.at[i], at(x, zt))

    def a_copy(q):
        return remote(abuf.at[pl.ds(0, depth)], abuf.at[pl.ds(q * depth, depth)],
                      a_s.at[q], a_r.at[q], at(xq(-q), z))

    def x_copy(i, q):
        rows = pl.ds(q * CAP, CAP)
        return remote(ssend.at[i, rows], srecv.at[i, rows], x_s.at[i, q], x_r.at[i, q], at(xq(q), z))

    def lg_copy(i, q):
        rows = pl.ds(q * depth, depth)
        return remote(lgs.at[i, rows], lgr.at[i, rows], lg_s.at[i, q], lg_r.at[i, q], at(xq(q), z))

    def o_copy(i, q):
        rows = pl.ds(q * CAP, CAP)
        return remote(osend.at[i, rows], oret.at[i, rows], o_s.at[i, q], o_r.at[i, q], at(xq(-q), z))

    def lr_copy(i, q):
        rows = pl.ds(q * depth, depth)
        return remote(lrs.at[i, rows], lrr.at[i, rows], lr_s.at[i, q], lr_r.at[i, q], at(xq(-q), z))

    def rs_copy(i):
        return remote(rss.at[i], rsr.at[i], r_s.at[i], r_r.at[i], at(x, ring(-out_step(i))))

    def go_copy(q):
        return remote(go.at[pl.ds(q * depth, depth)], gor.at[pl.ds(q * depth, depth)],
                      go_s.at[q], go_r.at[q], at(xq(q), z))

    def da_copy(r):
        kk, dev = peer(r)
        return remote(dpa.at[kk], dpr.at[r], da_s.at[r], da_r.at[r], dev)

    def db_copy():
        return remote(dpb, dpq, db_s, db_r, at(x, ring(ZL)))

    def dc_copy(r):
        _, dev = peer(r)
        return remote(dpo, dpf.at[r], dc_s.at[r], dc_r.at[r], dev)

    loads = [
        pltpu.make_async_copy(tok_hbm, tbuf.at[0], ld_sem.at[0]),
        pltpu.make_async_copy(au_hbm.at[0], abuf.at[pl.ds(0, depth)], ld_sem.at[1]),
        pltpu.make_async_copy(wg_hbm.at[0], wg, ld_sem.at[2]),
        pltpu.make_async_copy(wu_hbm.at[0], wu, ld_sem.at[3]),
        pltpu.make_async_copy(wd_hbm.at[0], wd, ld_sem.at[4]),
        pltpu.make_async_copy(ad_hbm.at[0], ad, ld_sem.at[5]),
        pltpu.make_async_copy(dy_hbm, dbuf.at[0], ld_sem.at[6]),
    ]
    for load in loads:
        load.start()

    barrier = pltpu.get_barrier_semaphore()
    friends = [at(x, ring(s)) for s in (1, -1, 2, -2, 3, -3, 4, -4)]
    friends += [at(xq(q), z) for q in range(1, XS)]
    friends += [peer(r)[1] for r in range(1, 2 * YS)]
    for friend in friends:
        pl.semaphore_signal(barrier, inc=1, device_id=friend, device_id_type=pl.DeviceIdType.MESH)

    ids_t = ids_ref[...].astype(F32)
    gates_t = gates_ref[...]
    slot = lax.broadcasted_iota(jnp.int32, (XS * ZL, 1), 0)
    owner = (lax.rem(x + lax.div(slot, ZL), XS) * ZL + lax.rem(slot, ZL)).astype(F32)
    gate_all = jnp.zeros((XS * ZL, toks), F32)
    hits = jnp.zeros((XS * ZL, toks), F32)
    for c in range(choices):
        hit = ids_t[c:c + 1] == owner
        gate_all += jnp.where(hit, gates_t[c:c + 1], 0.0)
        hits += hit.astype(F32)
    before = (lax.broadcasted_iota(jnp.int32, (toks, toks), 0)
              < lax.broadcasted_iota(jnp.int32, (toks, toks), 1)).astype(F32).astype(BF)
    rank_all = jnp.where(hits > 0.0, mm(hits.astype(BF), before), VOID)
    for q in range(XS):
        m_ref[:, q, :] = gate_all[q * ZL:(q + 1) * ZL]
        m_ref[:, XS + q, :] = rank_all[q * ZL:(q + 1) * ZL]
    mbuf[0] = m_ref[zl]
    gi[...] = jnp.zeros_like(gi)
    go[...] = jnp.zeros_like(go)
    loads[0].wait()
    pl.semaphore_wait(barrier, len(friends))

    for h in (0, 1):
        for i in (1, 2):
            tok_copy(i, h).start()
    for i in range(1, 8):
        m_copy(i).start()
    pl.semaphore_signal(far, inc=1, device_id=at(x, ring(-4)), device_id_type=pl.DeviceIdType.MESH)

    row_id = lax.broadcasted_iota(jnp.int32, (CAP, toks), 0).astype(F32)
    row_all = lax.broadcasted_iota(jnp.int32, (toks, toks), 0).astype(F32)
    lane_id = lax.broadcasted_iota(jnp.int32, (toks, ROWS), 1).astype(F32)

    def compact(i):
        m = mbuf[i]
        hot = jnp.concatenate(
            [(row_id == m[XS + q:XS + q + 1]).astype(F32) for q in range(XS)], axis=0).astype(BF)
        rows = mm(hot, tbuf[i]).astype(BF)
        srecv[i, 0:CAP] = rows[0:CAP]
        ssend[i, CAP:ROWS] = rows[CAP:ROWS]
        for q in range(1, XS):
            x_copy(i, q).start()

    def expert(i):
        for q in range(1, XS):
            x_copy(i, q).wait_recv()
        rows = srecv[i]
        g = mm_nt(rows, wg[...])
        u = mm_nt(rows, wu[...])
        h = (g / (1.0 + jnp.exp(-g)) * u).astype(BF)
        hbuf[i] = h
        adm = ad[...]
        low = mm_nt(h, adm).astype(BF)
        for q in range(XS):
            t = mm_nt(adm, h[q * CAP:(q + 1) * CAP]).astype(BF)
            if q == 0:
                lrr[i, 0:depth, 0:CAP] = t
            else:
                lrs[i, q * depth:(q + 1) * depth, 0:CAP] = t
        out = (mm(h, wd[...]) + mm(low, abuf[0:depth])).astype(BF)
        oret[i, 0:CAP] = out[0:CAP]
        osend[i, CAP:ROWS] = out[CAP:ROWS]
        for q in range(1, XS):
            lr_copy(i, q).start()

    def m_wait(i):
        remote(m_ref.at[0], mbuf.at[i], m_s.at[i], m_r.at[i], at(x, z)).wait_recv()

    def grad_in(n):
        for q in range(1, XS):
            lg_copy(n, q).wait_recv()
        acc = gi[:, 0:hidden]
        for q in range(XS):
            acc += mm(lgr[n, q * depth:(q + 1) * depth, 0:CAP], hbuf[n, q * CAP:(q + 1) * CAP])
        gi[:, 0:hidden] = acc

    def grads(n):
        m = mbuf[n]
        dy = dbuf[n]
        base = mm_nt(abuf[...], dy)
        lows = []
        for q in range(XS):
            gate = m[q:q + 1]
            rank = m[XS + q:XS + q + 1]
            lg = (base[q * depth:(q + 1) * depth] * gate).astype(BF)
            hot = (row_all == rank).astype(F32).astype(BF)
            packed = mm_nt(lg, hot).astype(BF)
            if q == 0:
                lgr[n, 0:depth] = packed
            else:
                lgs[n, q * depth:(q + 1) * depth] = packed
                lg_copy(n, q).start()
                lr_copy(n, q).wait_recv()
            low = mm(lrr[n, q * depth:(q + 1) * depth, 0:CAP], hot[0:CAP])
            lows.append((low * gate).astype(BF))
        go[...] += mm(jnp.concatenate(lows, axis=0), dy)

    def dy_in(i):
        dy_copy(i).wait_recv()
        if i + 2 <= 7:
            dy_copy(i + 2).start()

    compact(0)
    loads[1].wait()
    for q in range(1, XS):
        a_copy(q).start()
    for load in loads[2:]:
        load.wait()

    for pair in ((1, 2), (3, 4), (5, 6), (7,)):
        for h in (0, 1):
            for i in pair:
                tok_copy(i, h).wait_recv()
                if i + 2 <= 7:
                    tok_copy(i + 2, h).start()
        if pair == (3, 4):
            dy_copy(2).start()
        if pair == (5, 6):
            dy_copy(1).start()
        for i in pair:
            m_wait(i)
            compact(i)
        if pair == (1, 2):
            expert(0)
            for q in range(1, XS):
                a_copy(q).wait_recv()
        if pair == (3, 4):
            expert(1)
            expert(2)
            grads(0)
        if pair == (5, 6):
            expert(3)
            expert(4)
    dy_in(2)
    expert(5)
    for q in range(1, XS):
        o_copy(5, q).start()
    expert(6)
    for q in range(1, XS):
        o_copy(6, q).start()
    dy_in(1)
    expert(7)
    for q in range(1, XS):
        o_copy(7, q).start()

    def combine(i):
        for q in range(1, XS):
            o_copy(i, q).wait_recv()
        mt = mbuf[i].T
        wt = jnp.zeros((toks, ROWS), F32)
        for q in range(XS):
            wt = jnp.where(lane_id == mt[:, XS + q:XS + q + 1] + float(q * CAP), mt[:, q:q + 1], wt)
        hi = wt.astype(BF)
        lo = (wt - hi.astype(F32)).astype(BF)
        rows = oret[i]
        part = mm(hi, rows) + mm(lo, rows)
        if i >= 6:
            rss[i] = part.astype(BF)
        elif i >= 1:
            rs_copy(i + 2).wait_recv()
            rss[i] = (part + rsr[i + 2].astype(F32)).astype(BF)
        else:
            rs_copy(1).wait_recv()
            rs_copy(2).wait_recv()
            mixed_ref[...] = (part + rsr[1].astype(F32) + rsr[2].astype(F32)).astype(BF)
        if i >= 1:
            rs_copy(i).start()

    def returns(i):
        for q in range(1, XS):
            o_copy(i, q).start()

    def sum_a():
        for q in range(1, XS):
            go_copy(q).wait_recv()
        total = go[0:depth] + gor[depth:2 * depth] + gor[2 * depth:3 * depth] + gor[3 * depth:4 * depth]
        for j in range(2 * YS):
            cols = slice(j * 128, (j + 1) * 128)
            dpa[j, 0:depth] = total[:, cols]
            if j * 128 < hidden:
                dpa[j, depth:2 * depth] = gi[:, cols]
            else:
                dpa[j, depth:2 * depth] = jnp.zeros((depth, 128), F32)
        for r in range(1, 2 * YS):
            da_copy(r).start()

    def sum_b():
        own = dpa[k]
        for r in range(1, 2 * YS):
            da_copy(r).wait_recv()
            own += dpr[r]
        dpb[...] = own
        pl.semaphore_wait(far, 1)
        db_copy().start()

    def sum_c():
        db_copy().wait_recv()
        fin = (dpb[...] + dpq[...]).astype(BF)
        dpo[...] = fin
        dpf[0] = fin
        for r in range(1, 2 * YS):
            dc_copy(r).start()

    combine(7)
    returns(4)
    dy_in(4)
    dy_in(3)
    grads(2)
    combine(6)
    grads(1)
    returns(3)
    grads(4)
    combine(5)
    dy_in(6)
    dy_in(5)
    grads(3)
    returns(2)
    grad_in(0)
    grad_in(2)
    combine(4)
    grads(6)
    returns(1)
    grad_in(1)
    grad_in(4)
    combine(3)
    dy_in(7)
    grads(5)
    grads(7)
    for q in range(1, XS):
        go_copy(q).start()
    returns(0)
    grad_in(3)
    grad_in(6)
    combine(2)
    grad_in(5)
    combine(1)
    grad_in(7)
    sum_a()
    combine(0)
    sum_b()
    sum_c()
    for r in range(1, 2 * YS):
        dc_copy(r).wait_recv()
    for j in range(2 * YS):
        piece = dpf[lax.rem(k - j + 2 * YS, 2 * YS)]
        gout_ref[:, j * 128:(j + 1) * 128] = piece[0:depth]
        width = min(128, hidden - j * 128)
        if width > 0:
            gin_ref[:, j * 128:j * 128 + width] = piece[depth:2 * depth, 0:width]

    def drain(i, c):
        for q in range(1, XS):
            x_copy(i, q).wait_send()
            lg_copy(i, q).wait_send()
            o_copy(i, q).wait_send()
            lr_copy(i, q).wait_send()

        @pl.when(i >= 1)
        def _():
            for h in (0, 1):
                tok_copy(i, h).wait_send()
            dy_copy(i).wait_send()
            remote(m_ref.at[0], mbuf.at[i], m_s.at[i], m_r.at[i], at(x, z)).wait_send()
            rs_copy(i).wait_send()
            da_copy(i).wait_send()
            dc_copy(i).wait_send()

        return c

    lax.fori_loop(0, 8, drain, 0)
    db_copy().wait_send()
    for q in range(1, XS):
        a_copy(q).wait_send()
        go_copy(q).wait_send()


def settle(a_ref, b_ref, c_ref, ao_ref, bo_ref, co_ref):
    ao_ref[...] = a_ref[...]
    bo_ref[0] = b_ref[...]
    co_ref[0] = c_ref[...]


def shards(tokens, ids, gates, dy, wg, wu, wd, ad, au):
    toks, width = tokens.shape
    depth, hidden = ad.shape[1], ad.shape[2]
    anyspace = pl.BlockSpec(memory_space=pl.ANY)
    vmem = pl.BlockSpec(memory_space=pltpu.VMEM)
    dma = pltpu.SemaphoreType.DMA
    V = pltpu.VMEM
    mixed, gin, gout = pl.pallas_call(
        kernel,
        name="moe",
        out_shape=(
            jax.ShapeDtypeStruct((toks, width), BF),
            jax.ShapeDtypeStruct((depth, hidden), BF),
            jax.ShapeDtypeStruct((depth, width), BF),
        ),
        in_specs=[vmem, vmem] + [anyspace] * 7,
        out_specs=(vmem, vmem, vmem),
        scratch_shapes=[
            V((8, toks, width), BF), V((8, toks, width), BF), V((ZL, 2 * XS, toks), F32), V((8, 2 * XS, toks), F32),
            V((XS * depth, width), BF),
            V((hidden, width), BF), V((hidden, width), BF), V((hidden, width), BF), V((depth, hidden), BF),
            V((8, ROWS, width), BF), V((8, ROWS, width), BF), V((8, ROWS, hidden), BF),
            V((8, ROWS, width), BF), V((8, ROWS, width), BF),
            V((8, XS * depth, 128), BF), V((8, XS * depth, 128), BF),
            V((8, XS * depth, 128), BF), V((8, XS * depth, 128), BF),
            V((8, toks, width), BF), V((8, toks, width), BF),
            V((depth, 768), F32), V((XS * depth, width), F32), V((XS * depth, width), F32),
            V((8, 2 * depth, 128), F32), V((8, 2 * depth, 128), F32),
            V((2 * depth, 128), F32), V((2 * depth, 128), F32), V((2 * depth, 128), BF),
            V((8, 2 * depth, 128), BF),
            dma((7,)), dma((8, 2)), dma((8, 2)), dma((8,)), dma((8,)), dma((8,)), dma((8,)),
            dma((4,)), dma((4,)), dma((8, 4)), dma((8, 4)), dma((8, 4)), dma((8, 4)),
            dma((8, 4)), dma((8, 4)), dma((8, 4)), dma((8, 4)), dma((8,)), dma((8,)),
            dma((4,)), dma((4,)), dma((8,)), dma((8,)), dma(()), dma(()), dma((8,)), dma((8,)),
            pltpu.SemaphoreType.REGULAR,
        ],
        compiler_params=pltpu.CompilerParams(
            collective_id=0, has_side_effects=True, vmem_limit_bytes=61 * 1024 * 1024),
    )(ids.T, gates.T, tokens, dy, wg.swapaxes(1, 2), wu.swapaxes(1, 2), wd, ad, au)
    mixed, gin, gout = pl.pallas_call(
        settle,
        name="settle",
        out_shape=(
            jax.ShapeDtypeStruct((toks, width), BF),
            jax.ShapeDtypeStruct((1, depth, hidden), BF),
            jax.ShapeDtypeStruct((1, depth, width), BF),
        ),
        in_specs=[vmem] * 3,
        out_specs=(vmem, vmem, vmem),
    )(mixed, gin, gout)
    return mixed, gin, gout


def solution(mesh):
    tok = P(("dp", "expert"), None)
    exp = P("expert", None, None)
    return jax.shard_map(
        shards,
        mesh=mesh,
        in_specs=(tok, tok, tok, tok, exp, exp, exp, exp, exp),
        out_specs=(tok, exp, exp),
        check_vma=False,
    )
```

```python
import functools

import jax
import jax.numpy as jnp
from jax import lax
from jax.experimental import pallas as pl
from jax.experimental.pallas import tpu as pltpu
from jax.sharding import PartitionSpec as P

BF = jnp.bfloat16
F32 = jnp.float32
XS, ZL, ZS, YS = 4, 8, 16, 4
CAP = 48
ROWS = XS * CAP
VOID = -1000.0


def mm(a, b):
    return jnp.dot(a, b, preferred_element_type=F32)


def mm_nt(a, b):
    return lax.dot_general(a, b, (((1,), (1,)), ((), ())), preferred_element_type=F32)


def kernel(
    ids_hbm, gates_hbm, tok_hbm, dy_hbm, wg_hbm, wu_hbm, wd_hbm, ad_hbm, au_hbm,
    mixed_ref, gin_ref, gout_ref,
    tbuf, dbuf, own, idg, mbuf, abuf, wg, wu, wd, ad,
    ssend, srecv, hbuf, osend, oret, lgs, lgr, lrs, lrr, rss, rsr,
    gi, go, gob, gor, dpa, dpr, dpb, dpq, dpo, dpf,
    ld_sem, t_s, t_r, m_s, m_r, d_s, d_r, a_s, a_r, x_s, x_r, lg_s, lg_r,
    o_s, o_r, lr_s, lr_r, r_s, r_r, go_s, go_r, da_s, da_r, db_s, db_r, dc_s, dc_r, far,
):
    depth = ad_hbm.shape[1]
    hidden = wg_hbm.shape[1]
    choices = ids_hbm.shape[0]
    toks = tok_hbm.shape[0]
    half = toks // 2
    d = lax.axis_index("dp")
    e = lax.axis_index("expert")
    core = lax.rem(d, 2)
    y = lax.rem(lax.div(d, 2), YS)
    zh = lax.div(d, 2 * YS)
    x = lax.div(e, ZL)
    zl = lax.rem(e, ZL)
    z = zh * ZL + zl
    way = 1 - 2 * core
    k = y * 2 + core

    def at(x_, z_):
        return {"dp": lax.div(z_, ZL) * (2 * YS) + k, "expert": x_ * ZL + lax.rem(z_, ZL)}

    def ring(step):
        return lax.rem(z + step + ZS, ZS)

    def xq(q):
        return lax.rem(x + q + XS, XS)

    def peer(r):
        kk = lax.rem(k + r, 2 * YS)
        return kk, {"dp": zh * (2 * YS) + kk, "expert": e}

    def remote(src, dst, s, r, dev):
        return pltpu.make_async_remote_copy(
            src_ref=src, dst_ref=dst, send_sem=s, recv_sem=r,
            device_id=dev, device_id_type=pl.DeviceIdType.MESH)

    def group(ref, s):
        return remote(ref, ref, s, s, at(x, z))

    def three(ref, i, size):
        return ref.at[i, pl.ds(size, 3 * size)]

    def out_step(i):
        return way * (2 * lax.rem(i, 2) - 1)

    def tok_copy(i, h):
        src = jnp.maximum(i - 2, 0)
        rows = pl.ds(h * half, half)
        return remote(tbuf.at[src, rows], tbuf.at[i, rows], t_s.at[jnp.minimum(i, 2) - 1], t_r.at[i, h],
                      at(x, ring(out_step(i))))

    def dy_copy(i):
        src = jnp.maximum(i - 2, 0)
        return remote(dbuf.at[src], dbuf.at[i], d_s, d_r.at[i], at(x, ring(out_step(i))))

    def m_copy(i):
        src = jnp.maximum(i - 2, 0)
        return remote(idg.at[src], idg.at[i], m_s, m_r.at[i], at(x, ring(out_step(i))))

    def a_copy(q):
        return remote(abuf.at[pl.ds(0, depth)], abuf.at[pl.ds(q * depth, depth)],
                      a_s, a_r, at(xq(-q), z))

    def x_copy(i, q):
        rows = pl.ds(q * CAP, CAP)
        return remote(ssend.at[i, rows], srecv.at[i, rows], x_s, x_r.at[i], at(xq(q), z))

    def lg_copy(i, q):
        rows = pl.ds(q * depth, depth)
        return remote(lgs.at[i, rows], lgr.at[i, rows], lg_s, lg_r.at[i], at(xq(q), z))

    def o_copy(i, q):
        rows = pl.ds(q * CAP, CAP)
        return remote(osend.at[i, rows], oret.at[i, rows], o_s, o_r.at[i], at(xq(-q), z))

    def lr_copy(i, q):
        rows = pl.ds(q * depth, depth)
        return remote(lrs.at[i, rows], lrr.at[i, rows], lr_s, lr_r.at[i], at(xq(-q), z))

    def rs_copy(i, h):
        rows = pl.ds(h * half, half)
        return remote(rss.at[i, rows], rsr.at[i, rows], r_s, r_r.at[i, h],
                      at(x, ring(-out_step(i))))

    def go_copy(q):
        return remote(gob.at[pl.ds(q * depth, depth)], gor.at[pl.ds(q * depth, depth)],
                      go_s, go_r, at(xq(q), z))

    def da_copy(r):
        kk, dev = peer(r)
        return remote(dpa.at[kk], dpr.at[r], da_s, da_r, dev)

    def db_copy():
        return remote(dpb, dpq, db_s, db_r, at(x, ring(ZL)))

    def dc_copy(r):
        _, dev = peer(r)
        return remote(dpo, dpf.at[r], dc_s, dc_r, dev)

    loads = [
        pltpu.make_async_copy(tok_hbm, tbuf.at[0], ld_sem.at[0]),
        pltpu.make_async_copy(au_hbm.at[0], abuf.at[pl.ds(0, depth)], ld_sem.at[1]),
        pltpu.make_async_copy(wg_hbm.at[0], wg, ld_sem.at[2]),
        pltpu.make_async_copy(wu_hbm.at[0], wu, ld_sem.at[3]),
        pltpu.make_async_copy(wd_hbm.at[0], wd, ld_sem.at[4]),
        pltpu.make_async_copy(ad_hbm.at[0], ad, ld_sem.at[5]),
        pltpu.make_async_copy(dy_hbm, dbuf.at[0], ld_sem.at[6]),
        pltpu.make_async_copy(ids_hbm, own, ld_sem.at[7]),
        pltpu.make_async_copy(gates_hbm, idg.at[0, pl.ds(0, choices)], ld_sem.at[8]),
    ]
    barrier = pltpu.get_barrier_semaphore()
    friends = [at(x, ring(s)) for s in (1, -1)]
    friends += [at(xq(q), z) for q in range(1, XS)]
    friends += [peer(r)[1] for r in range(1, 2 * YS)]
    for friend in friends:
        pl.semaphore_signal(barrier, inc=1, device_id=friend, device_id_type=pl.DeviceIdType.MESH)
    for j in (0, 8, 7, 1, 6, 2, 3, 4, 5):
        loads[j].start()

    slot = lax.broadcasted_iota(jnp.int32, (XS, 1), 0)
    owner = (lax.rem(x + slot, XS) * ZL + zl).astype(F32)
    before = (lax.broadcasted_iota(jnp.int32, (toks, toks), 0)
              < lax.broadcasted_iota(jnp.int32, (toks, toks), 1)).astype(F32).astype(BF)
    gi[...] = jnp.zeros_like(gi)
    go[...] = jnp.zeros_like(go)
    loads[7].wait()
    loads[8].wait()
    idg[0, 8:8 + choices] = own[...].astype(F32)
    loads[0].wait()
    pl.semaphore_wait(barrier, len(friends))

    m_copy(1).start()
    for h in (0, 1):
        tok_copy(1, h).start()

    row_id = lax.broadcasted_iota(jnp.int32, (CAP, toks), 0).astype(F32)
    row_all = lax.broadcasted_iota(jnp.int32, (toks, toks), 0).astype(F32)
    lane_id = lax.broadcasted_iota(jnp.int32, (toks, ROWS), 1).astype(F32)

    def route(i):
        gate = jnp.zeros((XS, toks), F32)
        hits = jnp.zeros((XS, toks), F32)
        for c in range(choices):
            hit = idg[i, 8 + c:9 + c] == owner
            gate += jnp.where(hit, idg[i, c:c + 1], 0.0)
            hits += hit.astype(F32)
        m = jnp.concatenate([gate, jnp.where(hits > 0.0, mm(hits.astype(BF), before), VOID)], axis=0)
        mbuf[i] = m
        return m

    def compact(i):
        m = route(i)
        hot = jnp.concatenate(
            [(row_id == m[XS + q:XS + q + 1]).astype(F32) for q in range(XS)], axis=0).astype(BF)
        rows = mm(hot, tbuf[i]).astype(BF)
        srecv[i, 0:CAP] = rows[0:CAP]
        ssend[i, CAP:ROWS] = rows[CAP:ROWS]
        for q in range(1, XS):
            x_copy(i, q).start()

    def expert(i):
        group(three(srecv, i, CAP), x_r.at[i]).wait_recv()
        rows = srecv[i]
        g = mm_nt(rows, wg[...])
        u = mm_nt(rows, wu[...])
        h = (g / (1.0 + jnp.exp(-g)) * u).astype(BF)
        hbuf[i] = h
        adm = ad[...]
        low = mm_nt(h, adm).astype(BF)
        for q in range(XS):
            t = mm_nt(adm, h[q * CAP:(q + 1) * CAP]).astype(BF)
            if q == 0:
                lrr[i, 0:depth, 0:CAP] = t
            else:
                lrs[i, q * depth:(q + 1) * depth, 0:CAP] = t
        out = (mm(h, wd[...]) + mm(low, abuf[0:depth])).astype(BF)
        oret[i, 0:CAP] = out[0:CAP]
        osend[i, CAP:ROWS] = out[CAP:ROWS]
        for q in range(1, XS):
            lr_copy(i, q).start()

    def grad_in(n):
        group(three(lgr, n, depth), lg_r.at[n]).wait_recv()
        acc = gi[:, 0:hidden]
        for q in range(XS):
            acc += mm(lgr[n, q * depth:(q + 1) * depth, 0:CAP], hbuf[n, q * CAP:(q + 1) * CAP])
        gi[:, 0:hidden] = acc

    def grads(n):
        m = mbuf[n]
        dy = dbuf[n]
        base = mm_nt(abuf[...], dy)
        lows = []
        for q in range(XS):
            gate = m[q:q + 1]
            rank = m[XS + q:XS + q + 1]
            lg = (base[q * depth:(q + 1) * depth] * gate).astype(BF)
            hot = (row_all == rank).astype(F32).astype(BF)
            packed = mm_nt(lg, hot).astype(BF)
            if q == 0:
                lgr[n, 0:depth] = packed
            else:
                lgs[n, q * depth:(q + 1) * depth] = packed
                lg_copy(n, q).start()
            if q == 1:
                group(three(lrr, n, depth), lr_r.at[n]).wait_recv()
            low = mm(lrr[n, q * depth:(q + 1) * depth, 0:CAP], hot[0:CAP])
            lows.append((low * gate).astype(BF))
        go[...] += mm(jnp.concatenate(lows, axis=0), dy)

    def dy_in(i):
        dy_copy(i).wait_recv()
        if i + 2 <= 7:
            dy_copy(i + 2).start()

    def pass_on(i, h):
        if h == 0:
            m_copy(i).start()
        tok_copy(i, h).start()

    def tokens_in(i):
        m_copy(i).wait_recv()
        for h in (0, 1):
            tok_copy(i, h).wait_recv()
            if 1 < i <= 5:
                pass_on(i + 2, h)
        compact(i)
        if i == 1:
            pass_on(3, 0)
            pass_on(3, 1)

    def returns(i):
        for q in range(1, XS):
            o_copy(i, q).start()

    compact(0)
    group(tbuf.at[0], t_s.at[0]).wait_send()
    m_copy(2).start()
    for h in (0, 1):
        tok_copy(2, h).start()
    for j in (1, 6, 2, 3, 4, 5):
        loads[j].wait()
    for q in range(1, XS):
        a_copy(q).start()
    tokens_in(1)
    expert(0)
    tokens_in(2)
    tokens_in(3)
    dy_copy(1).start()
    expert(1)
    tokens_in(4)
    dy_copy(2).start()
    expert(2)
    tokens_in(5)
    expert(3)
    tokens_in(6)
    group(abuf.at[pl.ds(depth, 3 * depth)], a_r).wait_recv()
    grads(0)
    expert(4)
    tokens_in(7)
    pl.semaphore_signal(far, inc=1, device_id=at(x, ring(-4 * way)), device_id_type=pl.DeviceIdType.MESH)
    dy_in(1)
    dy_in(2)
    expert(5)
    grads(1)
    grads(2)
    expert(6)
    returns(6)
    dy_in(4)
    dy_in(3)
    expert(7)
    returns(7)
    returns(5)
    grads(4)
    grad_in(0)
    dy_in(6)
    grads(3)
    dy_in(5)
    grad_in(1)
    grad_in(2)

    def combine(i):
        group(three(oret, i, CAP), o_r.at[i]).wait_recv()
        mt = mbuf[i].T
        wt = jnp.zeros((toks, ROWS), F32)
        for q in range(XS):
            wt = jnp.where(lane_id == mt[:, XS + q:XS + q + 1] + float(q * CAP), mt[:, q:q + 1], wt)
        hi = wt.astype(BF)
        lo = (wt - hi.astype(F32)).astype(BF)
        rows = oret[i]
        for h in (0, 1):
            keep = slice(h * half, (h + 1) * half)
            both = mm(jnp.concatenate([hi[keep], lo[keep]], axis=0), rows)
            part = both[0:half] + both[half:]
            if i == 0:
                for j in (1, 2):
                    rs_copy(j, h).wait_recv()
                    part += rsr[j, keep].astype(F32)
                mixed_ref[keep] = part.astype(BF)
                continue
            if i < 6:
                rs_copy(i + 2, h).wait_recv()
                part += rsr[i + 2, keep].astype(F32)
            rss[i, keep] = part.astype(BF)
            rs_copy(i, h).start()

    def sum_a():
        group(gor.at[pl.ds(depth, 3 * depth)], go_r).wait_recv()
        total = go[0:depth]
        for q in range(1, XS):
            total += gor[q * depth:(q + 1) * depth].astype(F32)
        for j in range(2 * YS):
            cols = slice(j * 128, (j + 1) * 128)
            dpa[j, 0:depth] = total[:, cols]
            if j * 128 < hidden:
                dpa[j, depth:2 * depth] = gi[:, cols]
            else:
                dpa[j, depth:2 * depth] = jnp.zeros((depth, 128), F32)
        for r in range(1, 2 * YS):
            da_copy(r).start()

    def sum_b():
        mine = dpa[k]
        group(dpr.at[pl.ds(1, 2 * YS - 1)], da_r).wait_recv()
        for r in range(1, 2 * YS):
            mine += dpr[r]
        dpb[...] = mine
        pl.semaphore_wait(far, 1)
        db_copy().start()

    def sum_c():
        db_copy().wait_recv()
        fin = (dpb[...] + dpq[...]).astype(BF)
        dpo[...] = fin
        dpf[0] = fin
        for r in range(1, 2 * YS):
            dc_copy(r).start()

    combine(7)
    returns(4)
    grads(6)
    grads(5)
    combine(6)
    dy_in(7)
    grads(7)
    gob[...] = go[...].astype(BF)
    for q in range(1, XS):
        go_copy(q).start()
    returns(3)
    combine(5)
    returns(2)
    grad_in(4)
    grad_in(3)
    grad_in(6)
    grad_in(5)
    grad_in(7)
    sum_a()
    combine(4)
    returns(1)
    combine(3)
    returns(0)
    sum_b()
    combine(2)
    combine(1)
    sum_c()
    combine(0)
    group(dpf.at[pl.ds(1, 2 * YS - 1)], dc_r).wait_recv()
    for j in range(2 * YS):
        piece = dpf[lax.rem(k - j + 2 * YS, 2 * YS)]
        gout_ref[:, j * 128:(j + 1) * 128] = piece[0:depth]
        width = min(128, hidden - j * 128)
        if width > 0:
            gin_ref[:, j * 128:j * 128 + width] = piece[depth:2 * depth, 0:width]

    seven = pl.ds(1, 7)
    group(tbuf.at[pl.ds(2, 6)], t_s.at[1]).wait_send()
    group(idg.at[seven], m_s).wait_send()
    group(dbuf.at[seven], d_s).wait_send()
    group(rss.at[seven], r_s).wait_send()
    group(abuf.at[pl.ds(depth, 3 * depth)], a_s).wait_send()
    group(gob.at[pl.ds(depth, 3 * depth)], go_s).wait_send()
    group(ssend.at[:, pl.ds(CAP, 3 * CAP)], x_s).wait_send()
    group(osend.at[:, pl.ds(CAP, 3 * CAP)], o_s).wait_send()
    group(lgs.at[:, pl.ds(depth, 3 * depth)], lg_s).wait_send()
    group(lrs.at[:, pl.ds(depth, 3 * depth)], lr_s).wait_send()
    group(dpr.at[seven], da_s).wait_send()
    group(dpf.at[seven], dc_s).wait_send()
    db_copy().wait_send()


def settle(a_ref, b_ref, c_ref, ao_ref, bo_ref, co_ref):
    ao_ref[...] = a_ref[...]
    bo_ref[0] = b_ref[...]
    co_ref[0] = c_ref[...]


def shards(tokens, ids, gates, dy, wg, wu, wd, ad, au):
    toks, width = tokens.shape
    depth, hidden = ad.shape[1], ad.shape[2]
    anyspace = pl.BlockSpec(memory_space=pl.ANY)
    vmem = pl.BlockSpec(memory_space=pltpu.VMEM)
    dma = pltpu.SemaphoreType.DMA
    V = pltpu.VMEM
    mixed, gin, gout = pl.pallas_call(
        kernel,
        name="moe",
        out_shape=(
            jax.ShapeDtypeStruct((toks, width), BF),
            jax.ShapeDtypeStruct((depth, hidden), BF),
            jax.ShapeDtypeStruct((depth, width), BF),
        ),
        in_specs=[anyspace] * 9,
        out_specs=(vmem, vmem, vmem),
        scratch_shapes=[
            V((8, toks, width), BF), V((8, toks, width), BF), V(ids.shape[::-1], ids.dtype), V((8, 16, toks), F32),
            V((8, 2 * XS, toks), F32),
            V((XS * depth, width), BF),
            V((hidden, width), BF), V((hidden, width), BF), V((hidden, width), BF), V((depth, hidden), BF),
            V((8, ROWS, width), BF), V((8, ROWS, width), BF), V((8, ROWS, hidden), BF),
            V((8, ROWS, width), BF), V((8, ROWS, width), BF),
            V((8, XS * depth, 128), BF), V((8, XS * depth, 128), BF),
            V((8, XS * depth, 128), BF), V((8, XS * depth, 128), BF),
            V((8, toks, width), BF), V((8, toks, width), BF),
            V((depth, 768), F32), V((XS * depth, width), F32), V((XS * depth, width), BF), V((XS * depth, width), BF),
            V((8, 2 * depth, 128), F32), V((8, 2 * depth, 128), F32),
            V((2 * depth, 128), F32), V((2 * depth, 128), F32), V((2 * depth, 128), BF),
            V((8, 2 * depth, 128), BF),
            dma((9,)), dma((2,)), dma((8, 2)), dma(()), dma((8,)), dma(()), dma((8,)), dma(()), dma(()),
            dma(()), dma((8,)), dma(()), dma((8,)), dma(()), dma((8,)), dma(()), dma((8,)),
            dma(()), dma((8, 2)), dma(()), dma(()), dma(()), dma(()), dma(()), dma(()), dma(()), dma(()),
            pltpu.SemaphoreType.REGULAR,
        ],
        compiler_params=pltpu.CompilerParams(
            collective_id=0, has_side_effects=True, vmem_limit_bytes=61 * 1024 * 1024),
    )(ids.T, gates.T, tokens, dy, wg.swapaxes(1, 2), wu.swapaxes(1, 2), wd, ad, au)
    mixed, gin, gout = pl.pallas_call(
        settle,
        name="settle",
        out_shape=(
            jax.ShapeDtypeStruct((toks, width), BF),
            jax.ShapeDtypeStruct((1, depth, hidden), BF),
            jax.ShapeDtypeStruct((1, depth, width), BF),
        ),
        in_specs=[vmem] * 3,
        out_specs=(vmem, vmem, vmem),
    )(mixed, gin, gout)
    return mixed, gin, gout


def solution(mesh):
    tok = P(("dp", "expert"), None)
    exp = P("expert", None, None)
    return jax.shard_map(
        shards,
        mesh=mesh,
        in_specs=(tok, tok, tok, tok, exp, exp, exp, exp, exp),
        out_specs=(tok, exp, exp),
        check_vma=False,
    )
```

```python
import functools

import jax
import jax.numpy as jnp
from jax import lax
from jax.experimental import pallas as pl
from jax.experimental.pallas import tpu as pltpu
from jax.sharding import PartitionSpec as P

BF = jnp.bfloat16
F32 = jnp.float32
XS, ZL, ZS, YS = 4, 8, 16, 4
CAP = 48
ROWS = XS * CAP
VOID = -1000.0
TILE = (0, 1, 1, 2, 2, 3, 3, 4)
SIDE = (0, 0, 1, 1, 0, 1, 0, 0)


def mm(a, b):
    return jnp.dot(a, b, preferred_element_type=F32)


def mm_nt(a, b):
    return lax.dot_general(a, b, (((1,), (1,)), ((), ())), preferred_element_type=F32)


def kernel(
    ids_hbm, gates_hbm, tok_hbm, dy_hbm, wg_hbm, wu_hbm, wd_hbm, ad_hbm, au_hbm,
    mixed_ref, gin_ref, gout_ref,
    tbuf, dbuf, own, idg, mbuf, abuf, wg, wu, wd, ad,
    ssend, srecv, hbuf, osend, oret, lgs, lgr, lrs, lrr, rss, rsr,
    gi, go, gob, gor, dpa, dpr, dpb, dpq, dpo, dpf,
    ld_sem, t_s, t_r, m_s, m_r, d_s, d_r, a_s, a_r, x_s, x_r, lg_s, lg_r,
    o_s, o_r, lr_s, lr_r, r_s, r_r, go_s, go_r, da_s, da_r, db_s, db_r, dc_s, dc_r, far,
):
    depth = ad_hbm.shape[1]
    hidden = wg_hbm.shape[1]
    choices = ids_hbm.shape[0]
    toks = tok_hbm.shape[0]
    half = toks // 2
    d = lax.axis_index("dp")
    e = lax.axis_index("expert")
    core = lax.rem(d, 2)
    y = lax.rem(lax.div(d, 2), YS)
    zh = lax.div(d, 2 * YS)
    x = lax.div(e, ZL)
    zl = lax.rem(e, ZL)
    z = zh * ZL + zl
    way = 1 - 2 * core
    k = y * 2 + core

    def at(x_, z_):
        return {"dp": lax.div(z_, ZL) * (2 * YS) + k, "expert": x_ * ZL + lax.rem(z_, ZL)}

    def ring(step):
        return lax.rem(z + step + ZS, ZS)

    def xq(q):
        return lax.rem(x + q + XS, XS)

    def peer(r):
        kk = lax.rem(k + r, 2 * YS)
        return kk, {"dp": zh * (2 * YS) + kk, "expert": e}

    def remote(src, dst, s, r, dev):
        return pltpu.make_async_remote_copy(
            src_ref=src, dst_ref=dst, send_sem=s, recv_sem=r,
            device_id=dev, device_id_type=pl.DeviceIdType.MESH)

    def group(ref, s):
        return remote(ref, ref, s, s, at(x, z))

    def three(ref, i, size):
        return ref.at[i, pl.ds(size, 3 * size)]

    def out_step(i):
        return way * (2 * lax.rem(i, 2) - 1)

    def tok_copy(i, h):
        src = jnp.maximum(i - 2, 0)
        rows = pl.ds(h * half, half)
        return remote(tbuf.at[src, rows], tbuf.at[i, rows], t_s.at[jnp.minimum(i, 2) - 1], t_r.at[i, h],
                      at(x, ring(out_step(i))))

    def dy_copy(i):
        hops = 2 if i == 7 else 1
        return remote(dbuf.at[max(i - 2 * hops, 0)], dbuf.at[i], d_s, d_r.at[i],
                      at(x, ring(out_step(i) * hops)))

    def m_copy(i):
        src = jnp.maximum(i - 2, 0)
        return remote(idg.at[src], idg.at[i], m_s, m_r.at[i], at(x, ring(out_step(i))))

    def a_copy(q):
        return remote(abuf.at[pl.ds(0, depth)], abuf.at[pl.ds(q * depth, depth)],
                      a_s, a_r, at(xq(-q), z))

    def x_copy(i, q):
        rows = pl.ds(q * CAP, CAP)
        return remote(ssend.at[i, rows], srecv.at[i, rows], x_s, x_r.at[i], at(xq(q), z))

    def lg_copy(i, q):
        rows = pl.ds(q * depth, depth)
        return remote(lgs.at[i, rows], lgr.at[i, rows], lg_s, lg_r.at[i], at(xq(q), z))

    def o_copy(i, q):
        rows = pl.ds(q * CAP, CAP)
        return remote(osend.at[i, rows], oret.at[i, rows], o_s, o_r.at[i], at(xq(-q), z))

    def lr_copy(i, q):
        rows = pl.ds(q * depth, depth)
        return remote(lrs.at[i, rows], lrr.at[i, rows], lr_s, lr_r.at[i], at(xq(-q), z))

    def rs_copy(i, h):
        rows = pl.ds(h * half, half)
        return remote(rss.at[i, rows], rsr.at[i, rows], r_s, r_r.at[i, h],
                      at(x, ring(-out_step(i))))

    def go_copy(q):
        return remote(gob.at[pl.ds(q * depth, depth)], gor.at[pl.ds(q * depth, depth)],
                      go_s, go_r, at(xq(q), z))

    def da_copy(r):
        kk, dev = peer(r)
        return remote(dpa.at[kk], dpr.at[r], da_s, da_r, dev)

    def db_copy():
        return remote(dpb, dpq, db_s, db_r, at(x, ring(ZL)))

    def dc_copy(r):
        _, dev = peer(r)
        return remote(dpo, dpf.at[r], dc_s, dc_r, dev)

    loads = [
        pltpu.make_async_copy(tok_hbm, tbuf.at[0], ld_sem.at[0]),
        pltpu.make_async_copy(au_hbm.at[0], abuf.at[pl.ds(0, depth)], ld_sem.at[1]),
        pltpu.make_async_copy(wg_hbm.at[0], wg, ld_sem.at[2]),
        pltpu.make_async_copy(wu_hbm.at[0], wu, ld_sem.at[3]),
        pltpu.make_async_copy(wd_hbm.at[0], wd, ld_sem.at[4]),
        pltpu.make_async_copy(ad_hbm.at[0], ad, ld_sem.at[5]),
        pltpu.make_async_copy(dy_hbm, dbuf.at[0], ld_sem.at[6]),
        pltpu.make_async_copy(ids_hbm, own, ld_sem.at[7]),
        pltpu.make_async_copy(gates_hbm, idg.at[0, pl.ds(0, choices)], ld_sem.at[8]),
    ]
    barrier = pltpu.get_barrier_semaphore()
    friends = [at(x, ring(s)) for s in (1, -1)]
    friends += [at(xq(q), z) for q in range(1, XS)]
    friends += [peer(r)[1] for r in range(1, 2 * YS)]
    for friend in friends:
        pl.semaphore_signal(barrier, inc=1, device_id=friend, device_id_type=pl.DeviceIdType.MESH)
    for j in (0, 8, 7, 1, 6, 2, 3, 4, 5):
        loads[j].start()

    slot = lax.broadcasted_iota(jnp.int32, (XS, 1), 0)
    owner = (lax.rem(x + slot, XS) * ZL + zl).astype(F32)
    before = (lax.broadcasted_iota(jnp.int32, (toks, toks), 0)
              < lax.broadcasted_iota(jnp.int32, (toks, toks), 1)).astype(F32).astype(BF)
    gi[...] = jnp.zeros_like(gi)
    go[...] = jnp.zeros_like(go)
    loads[7].wait()
    loads[8].wait()
    idg[0, 8:8 + choices] = own[...].astype(F32)
    loads[0].wait()
    pl.semaphore_wait(barrier, len(friends))

    m_copy(1).start()
    for h in (0, 1):
        tok_copy(1, h).start()

    row_id = lax.broadcasted_iota(jnp.int32, (CAP, toks), 0).astype(F32)
    row_all = lax.broadcasted_iota(jnp.int32, (toks, toks), 0).astype(F32)
    lane_id = lax.broadcasted_iota(jnp.int32, (toks, ROWS), 1).astype(F32)

    def route(i):
        gate = jnp.zeros((XS, toks), F32)
        hits = jnp.zeros((XS, toks), F32)
        for c in range(choices):
            hit = idg[i, 8 + c:9 + c] == owner
            gate += jnp.where(hit, idg[i, c:c + 1], 0.0)
            hits += hit.astype(F32)
        m = jnp.concatenate([gate, jnp.where(hits > 0.0, mm(hits.astype(BF), before), VOID)], axis=0)
        mbuf[i] = m
        return m

    def compact(i):
        m = route(i)
        hot = jnp.concatenate(
            [(row_id == m[XS + q:XS + q + 1]).astype(F32) for q in range(XS)], axis=0).astype(BF)
        rows = mm(hot, tbuf[i]).astype(BF)
        srecv[i, 0:CAP] = rows[0:CAP]
        ssend[i, CAP:ROWS] = rows[CAP:ROWS]
        for q in range(1, XS):
            x_copy(i, q).start()

    def expert(i):
        group(three(srecv, i, CAP), x_r.at[i]).wait_recv()
        rows = srecv[i]
        g = mm_nt(rows, wg[...])
        u = mm_nt(rows, wu[...])
        h = (g / (1.0 + jnp.exp(-g)) * u).astype(BF)
        hbuf[i] = h
        adm = ad[...]
        low = mm_nt(h, adm).astype(BF)
        p, lanes = i // 2, slice(i % 2 * CAP, (i % 2 + 1) * CAP)
        for q in range(XS):
            t = mm_nt(adm, h[q * CAP:(q + 1) * CAP]).astype(BF)
            if q == 0:
                lrr[p, 0:depth, lanes] = t
            else:
                lrs[p, q * depth:(q + 1) * depth, lanes] = t
        out = (mm(h, wd[...]) + mm(low, abuf[0:depth])).astype(BF)
        oret[i, 0:CAP] = out[0:CAP]
        osend[i, CAP:ROWS] = out[CAP:ROWS]
        if i % 2 == 1:
            for q in range(1, XS):
                lr_copy(p, q).start()

    def grad_in(t):
        group(three(lgr, t, depth), lg_r.at[t]).wait_recv()
        acc = gi[:, 0:hidden]
        for n in range(8):
            if TILE[n] != t:
                continue
            lanes = slice(SIDE[n] * CAP, (SIDE[n] + 1) * CAP)
            for q in range(XS):
                acc += mm(lgr[t, q * depth:(q + 1) * depth, lanes], hbuf[n, q * CAP:(q + 1) * CAP])
        gi[:, 0:hidden] = acc

    seen_low = []
    seen_tile = []

    def grads(n):
        t, p = TILE[n], n // 2
        rows = slice(SIDE[n] * CAP, (SIDE[n] + 1) * CAP)
        lanes = slice(n % 2 * CAP, (n % 2 + 1) * CAP)
        if p not in seen_low:
            seen_low.append(p)
            group(three(lrr, p, depth), lr_r.at[p]).wait_recv()
        m = mbuf[n]
        dy = dbuf[n]
        base = mm_nt(abuf[...], dy)
        lows = []
        packs = []
        for q in range(XS):
            gate = m[q:q + 1]
            rank = m[XS + q:XS + q + 1]
            lg = (base[q * depth:(q + 1) * depth] * gate).astype(BF)
            hot = (row_all == rank + float(SIDE[n] * CAP)).astype(F32).astype(BF)
            packs.append(mm_nt(lg, hot))
            low = mm(lrr[p, q * depth:(q + 1) * depth, lanes], hot[rows])
            lows.append((low * gate).astype(BF))
        pack = jnp.concatenate(packs, axis=0)
        if t in seen_tile:
            pack += lgs[t].astype(F32)
        lgs[t] = pack.astype(BF)
        last = t in seen_tile or TILE.count(t) == 1
        seen_tile.append(t)
        if last:
            for q in range(1, XS):
                lg_copy(t, q).start()
            lgr[t, 0:depth] = pack[0:depth].astype(BF)
        go[...] += mm(jnp.concatenate(lows, axis=0), dy)

    def dy_in(i):
        dy_copy(i).wait_recv()
        if i <= 4:
            dy_copy(i + 2).start()
        if i == 3:
            dy_copy(7).start()

    def pass_on(i, h):
        if h == 0:
            m_copy(i).start()
        tok_copy(i, h).start()

    def tokens_in(i):
        m_copy(i).wait_recv()
        for h in (0, 1):
            tok_copy(i, h).wait_recv()
            if 1 < i <= 5:
                pass_on(i + 2, h)
        compact(i)
        if i == 1:
            pass_on(3, 0)
            pass_on(3, 1)

    def returns(i):
        for q in range(1, XS):
            o_copy(i, q).start()

    compact(0)
    group(tbuf.at[0], t_s.at[0]).wait_send()
    m_copy(2).start()
    for h in (0, 1):
        tok_copy(2, h).start()
    for j in (1, 6, 2, 3, 4, 5):
        loads[j].wait()
    for q in range(1, XS):
        a_copy(q).start()
    tokens_in(1)
    expert(0)
    tokens_in(2)
    tokens_in(3)
    dy_copy(1).start()
    expert(1)
    tokens_in(4)
    dy_copy(2).start()
    expert(2)
    tokens_in(5)
    expert(3)
    tokens_in(6)
    group(abuf.at[pl.ds(depth, 3 * depth)], a_r).wait_recv()
    grads(0)
    expert(4)
    dy_in(2)
    dy_in(1)
    tokens_in(7)
    pl.semaphore_signal(far, inc=1, device_id=at(x, ring(-4 * way)), device_id_type=pl.DeviceIdType.MESH)
    grads(1)
    grads(2)
    expert(5)
    expert(6)
    returns(6)
    dy_in(4)
    dy_in(3)
    expert(7)
    returns(7)
    returns(5)
    grads(4)
    grads(3)
    dy_in(6)
    grads(6)
    dy_in(5)
    grads(5)
    dy_in(7)
    grads(7)
    gob[...] = go[...].astype(BF)
    for q in range(1, XS):
        go_copy(q).start()

    def combine(i):
        group(three(oret, i, CAP), o_r.at[i]).wait_recv()
        mt = mbuf[i].T
        wt = jnp.zeros((toks, ROWS), F32)
        for q in range(XS):
            wt = jnp.where(lane_id == mt[:, XS + q:XS + q + 1] + float(q * CAP), mt[:, q:q + 1], wt)
        hi = wt.astype(BF)
        lo = (wt - hi.astype(F32)).astype(BF)
        rows = oret[i]
        for h in (0, 1):
            keep = slice(h * half, (h + 1) * half)
            both = mm(jnp.concatenate([hi[keep], lo[keep]], axis=0), rows)
            part = both[0:half] + both[half:]
            if i == 0:
                for j in (1, 2):
                    rs_copy(j, h).wait_recv()
                    part += rsr[j, keep].astype(F32)
                mixed_ref[keep] = part.astype(BF)
                continue
            if i < 6:
                rs_copy(i + 2, h).wait_recv()
                part += rsr[i + 2, keep].astype(F32)
            rss[i, keep] = part.astype(BF)
            rs_copy(i, h).start()

    def sum_a():
        group(gor.at[pl.ds(depth, 3 * depth)], go_r).wait_recv()
        total = go[0:depth]
        for q in range(1, XS):
            total += gor[q * depth:(q + 1) * depth].astype(F32)
        for j in range(2 * YS):
            cols = slice(j * 128, (j + 1) * 128)
            dpa[j, 0:depth] = total[:, cols]
            if j * 128 < hidden:
                dpa[j, depth:2 * depth] = gi[:, cols]
            else:
                dpa[j, depth:2 * depth] = jnp.zeros((depth, 128), F32)
        for r in range(1, 2 * YS):
            da_copy(r).start()

    def sum_b():
        mine = dpa[k]
        group(dpr.at[pl.ds(1, 2 * YS - 1)], da_r).wait_recv()
        for r in range(1, 2 * YS):
            mine += dpr[r]
        dpb[...] = mine
        pl.semaphore_wait(far, 1)
        db_copy().start()

    def sum_c():
        db_copy().wait_recv()
        fin = (dpb[...] + dpq[...]).astype(BF)
        dpo[...] = fin
        dpf[0] = fin
        for r in range(1, 2 * YS):
            dc_copy(r).start()

    combine(7)
    returns(4)
    grad_in(0)
    grad_in(1)
    combine(6)
    returns(3)
    grad_in(2)
    grad_in(3)
    grad_in(4)
    sum_a()
    combine(5)
    returns(2)
    sum_b()
    combine(4)
    returns(1)
    combine(3)
    returns(0)
    combine(2)
    sum_c()
    combine(1)
    combine(0)
    group(dpf.at[pl.ds(1, 2 * YS - 1)], dc_r).wait_recv()
    for j in range(2 * YS):
        piece = dpf[lax.rem(k - j + 2 * YS, 2 * YS)]
        gout_ref[:, j * 128:(j + 1) * 128] = piece[0:depth]
        width = min(128, hidden - j * 128)
        if width > 0:
            gin_ref[:, j * 128:j * 128 + width] = piece[depth:2 * depth, 0:width]

    seven = pl.ds(1, 7)
    group(tbuf.at[pl.ds(2, 6)], t_s.at[1]).wait_send()
    group(idg.at[seven], m_s).wait_send()
    group(dbuf.at[seven], d_s).wait_send()
    group(rss.at[seven], r_s).wait_send()
    group(abuf.at[pl.ds(depth, 3 * depth)], a_s).wait_send()
    group(gob.at[pl.ds(depth, 3 * depth)], go_s).wait_send()
    group(ssend.at[:, pl.ds(CAP, 3 * CAP)], x_s).wait_send()
    group(osend.at[:, pl.ds(CAP, 3 * CAP)], o_s).wait_send()
    group(lgs.at[:, pl.ds(depth, 3 * depth)], lg_s).wait_send()
    group(lrs.at[:, pl.ds(depth, 3 * depth)], lr_s).wait_send()
    group(dpr.at[seven], da_s).wait_send()
    group(dpf.at[seven], dc_s).wait_send()
    db_copy().wait_send()


def settle(a_ref, b_ref, c_ref, ao_ref, bo_ref, co_ref):
    ao_ref[...] = a_ref[...]
    bo_ref[0] = b_ref[...]
    co_ref[0] = c_ref[...]


def shards(tokens, ids, gates, dy, wg, wu, wd, ad, au):
    toks, width = tokens.shape
    depth, hidden = ad.shape[1], ad.shape[2]
    anyspace = pl.BlockSpec(memory_space=pl.ANY)
    vmem = pl.BlockSpec(memory_space=pltpu.VMEM)
    dma = pltpu.SemaphoreType.DMA
    V = pltpu.VMEM
    mixed, gin, gout = pl.pallas_call(
        kernel,
        name="moe",
        out_shape=(
            jax.ShapeDtypeStruct((toks, width), BF),
            jax.ShapeDtypeStruct((depth, hidden), BF),
            jax.ShapeDtypeStruct((depth, width), BF),
        ),
        in_specs=[anyspace] * 9,
        out_specs=(vmem, vmem, vmem),
        scratch_shapes=[
            V((8, toks, width), BF), V((8, toks, width), BF), V(ids.shape[::-1], ids.dtype), V((8, 16, toks), F32),
            V((8, 2 * XS, toks), F32),
            V((XS * depth, width), BF),
            V((hidden, width), BF), V((hidden, width), BF), V((hidden, width), BF), V((depth, hidden), BF),
            V((8, ROWS, width), BF), V((8, ROWS, width), BF), V((8, ROWS, hidden), BF),
            V((8, ROWS, width), BF), V((8, ROWS, width), BF),
            V((5, XS * depth, 128), BF), V((5, XS * depth, 128), BF),
            V((4, XS * depth, 128), BF), V((4, XS * depth, 128), BF),
            V((8, toks, width), BF), V((8, toks, width), BF),
            V((depth, 768), F32), V((XS * depth, width), F32), V((XS * depth, width), BF), V((XS * depth, width), BF),
            V((8, 2 * depth, 128), F32), V((8, 2 * depth, 128), F32),
            V((2 * depth, 128), F32), V((2 * depth, 128), F32), V((2 * depth, 128), BF),
            V((8, 2 * depth, 128), BF),
            dma((9,)), dma((2,)), dma((8, 2)), dma(()), dma((8,)), dma(()), dma((8,)), dma(()), dma(()),
            dma(()), dma((8,)), dma(()), dma((8,)), dma(()), dma((8,)), dma(()), dma((8,)),
            dma(()), dma((8, 2)), dma(()), dma(()), dma(()), dma(()), dma(()), dma(()), dma(()), dma(()),
            pltpu.SemaphoreType.REGULAR,
        ],
        compiler_params=pltpu.CompilerParams(
            collective_id=0, has_side_effects=True, vmem_limit_bytes=61 * 1024 * 1024),
    )(ids.T, gates.T, tokens, dy, wg.swapaxes(1, 2), wu.swapaxes(1, 2), wd, ad, au)
    mixed, gin, gout = pl.pallas_call(
        settle,
        name="settle",
        out_shape=(
            jax.ShapeDtypeStruct((toks, width), BF),
            jax.ShapeDtypeStruct((1, depth, hidden), BF),
            jax.ShapeDtypeStruct((1, depth, width), BF),
        ),
        in_specs=[vmem] * 3,
        out_specs=(vmem, vmem, vmem),
    )(mixed, gin, gout)
    return mixed, gin, gout


def solution(mesh):
    tok = P(("dp", "expert"), None)
    exp = P("expert", None, None)
    return jax.shard_map(
        shards,
        mesh=mesh,
        in_specs=(tok, tok, tok, tok, exp, exp, exp, exp, exp),
        out_specs=(tok, exp, exp),
        check_vma=False,
    )
```

```python
import functools

import jax
import jax.numpy as jnp
from jax import lax
from jax.experimental import pallas as pl
from jax.experimental.pallas import tpu as pltpu
from jax.sharding import PartitionSpec as P

BF = jnp.bfloat16
F32 = jnp.float32
XS, ZL, ZS, YS = 4, 8, 16, 4
CAP = 48
ROWS = XS * CAP
VOID = -1000.0
TILE = (0, 1, 1, 2, 2, 3, 3, 4)
SIDE = (0, 0, 1, 1, 0, 1, 0, 0)


def mm(a, b):
    return jnp.dot(a, b, preferred_element_type=F32)


def mm_nt(a, b):
    return lax.dot_general(a, b, (((1,), (1,)), ((), ())), preferred_element_type=F32)


def kernel(
    ids_hbm, gates_hbm, tok_hbm, dy_hbm, wg_hbm, wu_hbm, wd_hbm, ad_hbm, au_hbm,
    mixed_ref, gin_ref, gout_ref,
    tbuf, dbuf, own, idg, mbuf, abuf, wg, wu, wd, ad,
    ssend, srecv, hbuf, osend, oret, lgs, lgr, lrs, lrr, rss, rsr,
    gi, go, gob, gor, dpa, dpr, dpb, dpq, dpo, dpf,
    ld_sem, t_s, t_r, m_s, m_r, d_s, d_r, a_s, a_r, x_s, x_r, lg_s, lg_r,
    o_s, o_r, lr_s, lr_r, r_s, r_r, go_s, go_r, da_s, da_r, db_s, db_r, dc_s, dc_r, far,
):
    depth = ad_hbm.shape[1]
    hidden = wg_hbm.shape[1]
    choices = ids_hbm.shape[0]
    toks = tok_hbm.shape[0]
    half = toks // 2
    lead = toks // 4 * 3
    d = lax.axis_index("dp")
    e = lax.axis_index("expert")
    core = lax.rem(d, 2)
    y = lax.rem(lax.div(d, 2), YS)
    zh = lax.div(d, 2 * YS)
    x = lax.div(e, ZL)
    zl = lax.rem(e, ZL)
    z = zh * ZL + zl
    way = 1 - 2 * core
    k = y * 2 + core

    def at(x_, z_):
        return {"dp": lax.div(z_, ZL) * (2 * YS) + k, "expert": x_ * ZL + lax.rem(z_, ZL)}

    def ring(step):
        return lax.rem(z + step + ZS, ZS)

    def xq(q):
        return lax.rem(x + q + XS, XS)

    def peer(r):
        kk = lax.rem(k + r, 2 * YS)
        return kk, {"dp": zh * (2 * YS) + kk, "expert": e}

    def remote(src, dst, s, r, dev):
        return pltpu.make_async_remote_copy(
            src_ref=src, dst_ref=dst, send_sem=s, recv_sem=r,
            device_id=dev, device_id_type=pl.DeviceIdType.MESH)

    def group(ref, s):
        return remote(ref, ref, s, s, at(x, z))

    def three(ref, i, size):
        return ref.at[i, pl.ds(size, 3 * size)]

    def out_step(i):
        return way * (2 * lax.rem(i, 2) - 1)

    def tok_copy(i, h):
        src = max(i - 2, 0)
        rows = pl.ds(h * half, half)
        if i == 1:
            rows = pl.ds(h * lead, toks - lead if h else lead)
        return remote(tbuf.at[src, rows], tbuf.at[i, rows], t_s.at[h if i == 1 else 2], t_r.at[i, h],
                      at(x, ring(out_step(i))))

    def dy_copy(i):
        hops = 2 if i == 7 else 1
        return remote(dbuf.at[max(i - 2 * hops, 0)], dbuf.at[i], d_s, d_r.at[i],
                      at(x, ring(out_step(i) * hops)))

    def m_copy(i):
        src = jnp.maximum(i - 2, 0)
        return remote(idg.at[src], idg.at[i], m_s, m_r.at[i], at(x, ring(out_step(i))))

    def a_copy(q):
        return remote(abuf.at[pl.ds(0, depth)], abuf.at[pl.ds(q * depth, depth)],
                      a_s, a_r, at(xq(-q), z))

    def x_copy(i, q):
        rows = pl.ds(q * CAP, CAP)
        return remote(ssend.at[i, rows], srecv.at[i, rows], x_s, x_r.at[i], at(xq(q), z))

    def lg_copy(i, q):
        rows = pl.ds(q * depth, depth)
        return remote(lgs.at[i, rows], lgr.at[i, rows], lg_s, lg_r.at[i], at(xq(q), z))

    def o_copy(i, q):
        rows = pl.ds(q * CAP, CAP)
        return remote(osend.at[i, rows], oret.at[i, rows], o_s, o_r.at[i], at(xq(-q), z))

    def lr_copy(i, q):
        rows = pl.ds(q * depth, depth)
        return remote(lrs.at[i, rows], lrr.at[i, rows], lr_s, lr_r.at[i], at(xq(-q), z))

    def rs_copy(i, h):
        rows = pl.ds(h * half, half)
        return remote(rss.at[i, rows], rsr.at[i, rows], r_s, r_r.at[i, h],
                      at(x, ring(-out_step(i))))

    def go_copy(q):
        return remote(gob.at[pl.ds(q * depth, depth)], gor.at[pl.ds(q * depth, depth)],
                      go_s, go_r, at(xq(q), z))

    def da_copy(r):
        kk, dev = peer(r)
        return remote(dpa.at[kk], dpr.at[r], da_s, da_r, dev)

    def db_copy():
        return remote(dpb, dpq, db_s, db_r, at(x, ring(ZL)))

    def dc_copy(r):
        _, dev = peer(r)
        return remote(dpo, dpf.at[r], dc_s, dc_r, dev)

    loads = [
        pltpu.make_async_copy(tok_hbm, tbuf.at[0], ld_sem.at[0]),
        pltpu.make_async_copy(au_hbm.at[0], abuf.at[pl.ds(0, depth)], ld_sem.at[1]),
        pltpu.make_async_copy(wg_hbm.at[0], wg, ld_sem.at[2]),
        pltpu.make_async_copy(wu_hbm.at[0], wu, ld_sem.at[3]),
        pltpu.make_async_copy(wd_hbm.at[0], wd, ld_sem.at[4]),
        pltpu.make_async_copy(ad_hbm.at[0], ad, ld_sem.at[5]),
        pltpu.make_async_copy(dy_hbm, dbuf.at[0], ld_sem.at[6]),
        pltpu.make_async_copy(ids_hbm, own, ld_sem.at[7]),
        pltpu.make_async_copy(gates_hbm, idg.at[0, pl.ds(0, choices)], ld_sem.at[8]),
    ]
    barrier = pltpu.get_barrier_semaphore()
    friends = [at(x, ring(s)) for s in (1, -1)]
    friends += [at(xq(q), z) for q in range(1, XS)]
    friends += [peer(r)[1] for r in range(1, 2 * YS)]
    for friend in friends:
        pl.semaphore_signal(barrier, inc=1, device_id=friend, device_id_type=pl.DeviceIdType.MESH)
    for j in (0, 8, 7, 1, 6, 2, 3, 4, 5):
        loads[j].start()

    slot = lax.broadcasted_iota(jnp.int32, (XS, 1), 0)
    owner = (lax.rem(x + slot, XS) * ZL + zl).astype(F32)
    before = (lax.broadcasted_iota(jnp.int32, (toks, toks), 0)
              < lax.broadcasted_iota(jnp.int32, (toks, toks), 1)).astype(F32).astype(BF)
    gi[...] = jnp.zeros_like(gi)
    go[...] = jnp.zeros_like(go)
    loads[7].wait()
    loads[8].wait()
    idg[0, 8:8 + choices] = own[...].astype(F32)
    loads[0].wait()
    pl.semaphore_wait(barrier, len(friends))

    m_copy(1).start()
    for h in (0, 1):
        tok_copy(1, h).start()

    row_id = lax.broadcasted_iota(jnp.int32, (CAP, toks), 0).astype(F32)
    row_all = lax.broadcasted_iota(jnp.int32, (toks, toks), 0).astype(F32)
    lane_id = lax.broadcasted_iota(jnp.int32, (toks, ROWS), 1).astype(F32)

    def route(i):
        gate = jnp.zeros((XS, toks), F32)
        hits = jnp.zeros((XS, toks), F32)
        for c in range(choices):
            hit = idg[i, 8 + c:9 + c] == owner
            gate += jnp.where(hit, idg[i, c:c + 1], 0.0)
            hits += hit.astype(F32)
        m = jnp.concatenate([gate, jnp.where(hits > 0.0, mm(hits.astype(BF), before), VOID)], axis=0)
        mbuf[i] = m
        return m

    def compact(i):
        m = route(i)
        hot = jnp.concatenate(
            [(row_id == m[XS + q:XS + q + 1]).astype(F32) for q in range(XS)], axis=0).astype(BF)
        rows = mm(hot, tbuf[i]).astype(BF)
        srecv[i, 0:CAP] = rows[0:CAP]
        ssend[i, CAP:ROWS] = rows[CAP:ROWS]
        for q in range(1, XS):
            x_copy(i, q).start()

    def expert(i):
        group(three(srecv, i, CAP), x_r.at[i]).wait_recv()
        rows = srecv[i]
        g = mm_nt(rows, wg[...])
        u = mm_nt(rows, wu[...])
        h = (g / (1.0 + jnp.exp(-g)) * u).astype(BF)
        hbuf[i] = h
        adm = ad[...]
        low = mm_nt(h, adm).astype(BF)
        p, lanes = i // 2, slice(i % 2 * CAP, (i % 2 + 1) * CAP)
        for q in range(XS):
            t = mm_nt(adm, h[q * CAP:(q + 1) * CAP]).astype(BF)
            if q == 0:
                lrr[p, 0:depth, lanes] = t
            else:
                lrs[p, q * depth:(q + 1) * depth, lanes] = t
        out = (mm(h, wd[...]) + mm(low, abuf[0:depth])).astype(BF)
        oret[i, 0:CAP] = out[0:CAP]
        osend[i, CAP:ROWS] = out[CAP:ROWS]
        if i % 2 == 1:
            for q in range(1, XS):
                lr_copy(p, q).start()

    def grad_in(t):
        group(three(lgr, t, depth), lg_r.at[t]).wait_recv()
        acc = gi[:, 0:hidden]
        for n in range(8):
            if TILE[n] != t:
                continue
            lanes = slice(SIDE[n] * CAP, (SIDE[n] + 1) * CAP)
            for q in range(XS):
                acc += mm(lgr[t, q * depth:(q + 1) * depth, lanes], hbuf[n, q * CAP:(q + 1) * CAP])
        gi[:, 0:hidden] = acc

    seen_low = []
    seen_tile = []

    def grads(n):
        t, p = TILE[n], n // 2
        rows = slice(SIDE[n] * CAP, (SIDE[n] + 1) * CAP)
        lanes = slice(n % 2 * CAP, (n % 2 + 1) * CAP)
        if p not in seen_low:
            seen_low.append(p)
            group(three(lrr, p, depth), lr_r.at[p]).wait_recv()
        m = mbuf[n]
        dy = dbuf[n]
        base = mm_nt(abuf[...], dy)
        lows = []
        packs = []
        for q in range(XS):
            gate = m[q:q + 1]
            rank = m[XS + q:XS + q + 1]
            lg = (base[q * depth:(q + 1) * depth] * gate).astype(BF)
            hot = (row_all == rank + float(SIDE[n] * CAP)).astype(F32).astype(BF)
            packs.append(mm_nt(lg, hot))
            low = mm(lrr[p, q * depth:(q + 1) * depth, lanes], hot[rows])
            lows.append((low * gate).astype(BF))
        pack = jnp.concatenate(packs, axis=0)
        if t in seen_tile:
            pack += lgs[t].astype(F32)
        lgs[t] = pack.astype(BF)
        last = t in seen_tile or TILE.count(t) == 1
        seen_tile.append(t)
        if last:
            for q in range(1, XS):
                lg_copy(t, q).start()
            lgr[t, 0:depth] = pack[0:depth].astype(BF)
        go[...] += mm(jnp.concatenate(lows, axis=0), dy)

    def dy_in(i):
        dy_copy(i).wait_recv()
        if i <= 4:
            dy_copy(i + 2).start()
        if i == 3:
            dy_copy(7).start()

    def pass_on(i, h):
        if h == 0:
            m_copy(i).start()
        tok_copy(i, h).start()

    def tokens_in(i):
        m_copy(i).wait_recv()
        for h in (0, 1):
            tok_copy(i, h).wait_recv()
            if 1 < i <= 5:
                pass_on(i + 2, h)
        compact(i)
        if i == 1:
            pass_on(3, 0)
            pass_on(3, 1)

    def returns(i):
        for q in range(1, XS):
            o_copy(i, q).start()

    compact(0)
    group(tbuf.at[0, pl.ds(0, lead)], t_s.at[0]).wait_send()
    m_copy(2).start()
    for h in (0, 1):
        tok_copy(2, h).start()
    for j in (1, 6, 2, 3, 4, 5):
        loads[j].wait()
    for q in range(1, XS):
        a_copy(q).start()
    tokens_in(1)
    expert(0)
    tokens_in(2)
    tokens_in(3)
    dy_copy(1).start()
    expert(1)
    tokens_in(4)
    dy_copy(2).start()
    expert(2)
    tokens_in(5)
    expert(3)
    tokens_in(6)
    group(abuf.at[pl.ds(depth, 3 * depth)], a_r).wait_recv()
    grads(0)
    expert(4)
    dy_in(2)
    dy_in(1)
    tokens_in(7)
    pl.semaphore_signal(far, inc=1, device_id=at(x, ring(-4 * way)), device_id_type=pl.DeviceIdType.MESH)
    grads(1)
    grads(2)
    expert(5)
    expert(6)
    returns(6)
    dy_in(4)
    dy_in(3)
    expert(7)
    returns(7)
    returns(5)
    grads(4)
    grads(3)
    dy_in(6)
    grads(6)
    dy_in(5)
    grads(5)
    dy_in(7)
    grads(7)
    gob[...] = go[...].astype(BF)
    for q in range(1, XS):
        go_copy(q).start()
    returns(4)

    def combine(i):
        group(three(oret, i, CAP), o_r.at[i]).wait_recv()
        mt = mbuf[i].T
        wt = jnp.zeros((toks, ROWS), F32)
        for q in range(XS):
            wt = jnp.where(lane_id == mt[:, XS + q:XS + q + 1] + float(q * CAP), mt[:, q:q + 1], wt)
        hi = wt.astype(BF)
        lo = (wt - hi.astype(F32)).astype(BF)
        rows = oret[i]
        for h in (0, 1):
            keep = slice(h * half, (h + 1) * half)
            both = mm(jnp.concatenate([hi[keep], lo[keep]], axis=0), rows)
            part = both[0:half] + both[half:]
            if i == 0:
                for j in (1, 2):
                    rs_copy(j, h).wait_recv()
                    part += rsr[j, keep].astype(F32)
                mixed_ref[keep] = part.astype(BF)
                continue
            if i < 6:
                rs_copy(i + 2, h).wait_recv()
                part += rsr[i + 2, keep].astype(F32)
            rss[i, keep] = part.astype(BF)
            rs_copy(i, h).start()

    def sum_a():
        group(gor.at[pl.ds(depth, 3 * depth)], go_r).wait_recv()
        total = go[0:depth]
        for q in range(1, XS):
            total += gor[q * depth:(q + 1) * depth].astype(F32)
        for j in range(2 * YS):
            cols = slice(j * 128, (j + 1) * 128)
            dpa[j, 0:depth] = total[:, cols]
            if j * 128 < hidden:
                dpa[j, depth:2 * depth] = gi[:, cols]
            else:
                dpa[j, depth:2 * depth] = jnp.zeros((depth, 128), F32)
        for r in range(1, 2 * YS):
            da_copy(r).start()

    def sum_b():
        mine = dpa[k]
        group(dpr.at[pl.ds(1, 2 * YS - 1)], da_r).wait_recv()
        for r in range(1, 2 * YS):
            mine += dpr[r]
        dpb[...] = mine
        pl.semaphore_wait(far, 1)
        db_copy().start()

    def sum_c():
        db_copy().wait_recv()
        fin = (dpb[...] + dpq[...]).astype(BF)
        dpo[...] = fin
        dpf[0] = fin
        for r in range(1, 2 * YS):
            dc_copy(r).start()

    combine(7)
    grad_in(0)
    grad_in(1)
    combine(6)
    returns(3)
    grad_in(2)
    grad_in(3)
    grad_in(4)
    sum_a()
    combine(5)
    returns(2)
    sum_b()
    combine(4)
    returns(1)
    combine(3)
    returns(0)
    combine(2)
    sum_c()
    combine(1)
    combine(0)
    group(dpf.at[pl.ds(1, 2 * YS - 1)], dc_r).wait_recv()
    for j in range(2 * YS):
        piece = dpf[lax.rem(k - j + 2 * YS, 2 * YS)]
        gout_ref[:, j * 128:(j + 1) * 128] = piece[0:depth]
        width = min(128, hidden - j * 128)
        if width > 0:
            gin_ref[:, j * 128:j * 128 + width] = piece[depth:2 * depth, 0:width]

    seven = pl.ds(1, 7)
    group(tbuf.at[0, pl.ds(lead, toks - lead)], t_s.at[1]).wait_send()
    group(tbuf.at[pl.ds(2, 6)], t_s.at[2]).wait_send()
    group(idg.at[seven], m_s).wait_send()
    group(dbuf.at[seven], d_s).wait_send()
    group(rss.at[seven], r_s).wait_send()
    group(abuf.at[pl.ds(depth, 3 * depth)], a_s).wait_send()
    group(gob.at[pl.ds(depth, 3 * depth)], go_s).wait_send()
    group(ssend.at[:, pl.ds(CAP, 3 * CAP)], x_s).wait_send()
    group(osend.at[:, pl.ds(CAP, 3 * CAP)], o_s).wait_send()
    group(lgs.at[:, pl.ds(depth, 3 * depth)], lg_s).wait_send()
    group(lrs.at[:, pl.ds(depth, 3 * depth)], lr_s).wait_send()
    group(dpr.at[seven], da_s).wait_send()
    group(dpf.at[seven], dc_s).wait_send()
    db_copy().wait_send()


def settle(a_ref, b_ref, c_ref, ao_ref, bo_ref, co_ref):
    ao_ref[...] = a_ref[...]
    bo_ref[0] = b_ref[...]
    co_ref[0] = c_ref[...]


def shards(tokens, ids, gates, dy, wg, wu, wd, ad, au):
    toks, width = tokens.shape
    depth, hidden = ad.shape[1], ad.shape[2]
    hbm = pl.BlockSpec(memory_space=pltpu.HBM)
    vmem = pl.BlockSpec(memory_space=pltpu.VMEM)
    dma = pltpu.SemaphoreType.DMA
    V = pltpu.VMEM
    mixed, gin, gout = pl.pallas_call(
        kernel,
        name="moe",
        out_shape=(
            jax.ShapeDtypeStruct((toks, width), BF),
            jax.ShapeDtypeStruct((depth, hidden), BF),
            jax.ShapeDtypeStruct((depth, width), BF),
        ),
        in_specs=[hbm] * 9,
        out_specs=(vmem, vmem, vmem),
        scratch_shapes=[
            V((8, toks, width), BF), V((8, toks, width), BF), V(ids.shape[::-1], ids.dtype), V((8, 16, toks), F32),
            V((8, 2 * XS, toks), F32),
            V((XS * depth, width), BF),
            V((hidden, width), BF), V((hidden, width), BF), V((hidden, width), BF), V((depth, hidden), BF),
            V((8, ROWS, width), BF), V((8, ROWS, width), BF), V((8, ROWS, hidden), BF),
            V((8, ROWS, width), BF), V((8, ROWS, width), BF),
            V((5, XS * depth, 128), BF), V((5, XS * depth, 128), BF),
            V((4, XS * depth, 128), BF), V((4, XS * depth, 128), BF),
            V((8, toks, width), BF), V((8, toks, width), BF),
            V((depth, 768), F32), V((XS * depth, width), F32), V((XS * depth, width), BF), V((XS * depth, width), BF),
            V((8, 2 * depth, 128), F32), V((8, 2 * depth, 128), F32),
            V((2 * depth, 128), F32), V((2 * depth, 128), F32), V((2 * depth, 128), BF),
            V((8, 2 * depth, 128), BF),
            dma((9,)), dma((3,)), dma((8, 2)), dma(()), dma((8,)), dma(()), dma((8,)), dma(()), dma(()),
            dma(()), dma((8,)), dma(()), dma((8,)), dma(()), dma((8,)), dma(()), dma((8,)),
            dma(()), dma((8, 2)), dma(()), dma(()), dma(()), dma(()), dma(()), dma(()), dma(()), dma(()),
            pltpu.SemaphoreType.REGULAR,
        ],
        compiler_params=pltpu.CompilerParams(
            collective_id=0, has_side_effects=True, vmem_limit_bytes=48 * 1024 * 1024),
    )(*(pltpu.with_memory_space_constraint(v, pltpu.HBM) for v in (
        ids.T, gates.T, tokens, dy, wg.swapaxes(1, 2), wu.swapaxes(1, 2), wd, ad, au)))
    mixed, gin, gout = pl.pallas_call(
        settle,
        name="settle",
        out_shape=(
            jax.ShapeDtypeStruct((toks, width), BF),
            jax.ShapeDtypeStruct((1, depth, hidden), BF),
            jax.ShapeDtypeStruct((1, depth, width), BF),
        ),
        in_specs=[vmem] * 3,
        out_specs=(vmem, vmem, vmem),
        compiler_params=pltpu.CompilerParams(vmem_limit_bytes=4 * 1024 * 1024),
    )(mixed, gin, gout)
    return mixed, gin, gout


def solution(mesh):
    tok = P(("dp", "expert"), None)
    exp = P("expert", None, None)
    return jax.shard_map(
        shards,
        mesh=mesh,
        in_specs=(tok, tok, tok, tok, exp, exp, exp, exp, exp),
        out_specs=(tok, exp, exp),
        check_vma=False,
    )
```

```python
import functools

import jax
import jax.numpy as jnp
from jax import lax
from jax.experimental import pallas as pl
from jax.experimental.pallas import tpu as pltpu
from jax.sharding import PartitionSpec as P

BF = jnp.bfloat16
F32 = jnp.float32
XS, ZL, ZS, YS = 4, 8, 16, 4
CAP = 48
ROWS = XS * CAP
VOID = -1000.0
TILE = (0, 1, 1, 2, 2, 3, 3, 4)
SIDE = (0, 0, 1, 1, 0, 1, 0, 0)


def mm(a, b):
    return jnp.dot(a, b, preferred_element_type=F32)


def mm_nt(a, b):
    return lax.dot_general(a, b, (((1,), (1,)), ((), ())), preferred_element_type=F32)


def kernel(
    ids_hbm, gates_hbm, tok_hbm, dy_hbm, wg_hbm, wu_hbm, wd_hbm, ad_hbm, au_hbm,
    mixed_ref, gin_ref, gout_ref,
    tbuf, dbuf, own, idg, mbuf, abuf, wg, wu, wd, ad,
    ssend, srecv, hbuf, osend, oret, lgs, lgr, lrs, lrr, rss, rsr,
    gi, go, goc, goy, gox, gor, dpa, dpr, dpb, dpq, dpo, dpf,
    ld_sem, t_s, t_r, m_s, m_r, d_s, d_r, a_s, a_r, x_s, x_r, lg_s, lg_r,
    o_s, o_r, lr_s, lr_r, r_s, r_r, go_s, go_r, gy_s, gy_r, da_s, da_r, db_s, db_r, dc_s, dc_r, far,
):
    depth = ad_hbm.shape[1]
    hidden = wg_hbm.shape[1]
    choices = ids_hbm.shape[0]
    toks = tok_hbm.shape[0]
    half = toks // 2
    lead = toks // 4 * 3
    d = lax.axis_index("dp")
    e = lax.axis_index("expert")
    core = lax.rem(d, 2)
    y = lax.rem(lax.div(d, 2), YS)
    zh = lax.div(d, 2 * YS)
    x = lax.div(e, ZL)
    zl = lax.rem(e, ZL)
    z = zh * ZL + zl
    way = 1 - 2 * core
    k = y * 2 + core

    def at(x_, z_):
        return {"dp": lax.div(z_, ZL) * (2 * YS) + k, "expert": x_ * ZL + lax.rem(z_, ZL)}

    def ring(step):
        return lax.rem(z + step + ZS, ZS)

    def xq(q):
        return lax.rem(x + q + XS, XS)

    def peer(r):
        kk = lax.rem(k + r, 2 * YS)
        return kk, {"dp": zh * (2 * YS) + kk, "expert": e}

    def remote(src, dst, s, r, dev):
        return pltpu.make_async_remote_copy(
            src_ref=src, dst_ref=dst, send_sem=s, recv_sem=r,
            device_id=dev, device_id_type=pl.DeviceIdType.MESH)

    def group(ref, s):
        return remote(ref, ref, s, s, at(x, z))

    def three(ref, i, size):
        return ref.at[i, pl.ds(size, 3 * size)]

    def out_step(i):
        return way * (2 * lax.rem(i, 2) - 1)

    def tok_copy(i, h):
        src = max(i - 2, 0)
        rows = pl.ds(h * half, half)
        if i == 1:
            rows = pl.ds(h * lead, toks - lead if h else lead)
        return remote(tbuf.at[src, rows], tbuf.at[i, rows], t_s.at[h if i == 1 else 2], t_r.at[i, h],
                      at(x, ring(out_step(i))))

    def dy_copy(i):
        hops = 2 if i == 7 else 1
        return remote(dbuf.at[max(i - 2 * hops, 0)], dbuf.at[i], d_s, d_r.at[i],
                      at(x, ring(out_step(i) * hops)))

    def m_copy(i):
        src = jnp.maximum(i - 2, 0)
        return remote(idg.at[src], idg.at[i], m_s, m_r.at[i], at(x, ring(out_step(i))))

    def a_copy(q):
        return remote(abuf.at[pl.ds(0, depth)], abuf.at[pl.ds(q * depth, depth)],
                      a_s, a_r, at(xq(-q), z))

    def x_copy(i, q):
        rows = pl.ds(q * CAP, CAP)
        return remote(ssend.at[i, rows], srecv.at[i, rows], x_s, x_r.at[i], at(xq(q), z))

    def lg_copy(i, q):
        rows = pl.ds(q * depth, depth)
        return remote(lgs.at[i, rows], lgr.at[i, rows], lg_s, lg_r.at[i], at(xq(q), z))

    def o_copy(i, q):
        rows = pl.ds(q * CAP, CAP)
        return remote(osend.at[i, rows], oret.at[i, rows], o_s, o_r.at[i], at(xq(-q), z))

    def lr_copy(i, q):
        rows = pl.ds(q * depth, depth)
        return remote(lrs.at[i, rows], lrr.at[i, rows], lr_s, lr_r.at[i], at(xq(-q), z))

    def rs_copy(i, h):
        rows = pl.ds(h * half, half)
        return remote(rss.at[i, rows], rsr.at[i, rows], r_s, r_r.at[i, h],
                      at(x, ring(-out_step(i))))

    def go_copy(q):
        return remote(gox.at[pl.ds(q * depth, depth)], gor.at[pl.ds(q * depth, depth)],
                      go_s, go_r, at(xq(q), z))

    def gy_copy(r):
        kk, dev = peer(r)
        return remote(goc.at[kk], goy.at[r], gy_s, gy_r, dev)

    def da_copy(r):
        kk, dev = peer(r)
        return remote(dpa.at[kk], dpr.at[r], da_s, da_r, dev)

    def db_copy():
        return remote(dpb, dpq, db_s, db_r, at(x, ring(ZL)))

    def dc_copy(r):
        _, dev = peer(r)
        return remote(dpo, dpf.at[r], dc_s, dc_r, dev)

    loads = [
        pltpu.make_async_copy(tok_hbm, tbuf.at[0], ld_sem.at[0]),
        pltpu.make_async_copy(au_hbm.at[0], abuf.at[pl.ds(0, depth)], ld_sem.at[1]),
        pltpu.make_async_copy(wg_hbm.at[0], wg, ld_sem.at[2]),
        pltpu.make_async_copy(wu_hbm.at[0], wu, ld_sem.at[3]),
        pltpu.make_async_copy(wd_hbm.at[0], wd, ld_sem.at[4]),
        pltpu.make_async_copy(ad_hbm.at[0], ad, ld_sem.at[5]),
        pltpu.make_async_copy(dy_hbm, dbuf.at[0], ld_sem.at[6]),
        pltpu.make_async_copy(ids_hbm, own, ld_sem.at[7]),
        pltpu.make_async_copy(gates_hbm, idg.at[0, pl.ds(0, choices)], ld_sem.at[8]),
    ]
    barrier = pltpu.get_barrier_semaphore()
    friends = [at(x, ring(s)) for s in (1, -1)]
    friends += [at(xq(q), z) for q in range(1, XS)]
    friends += [peer(r)[1] for r in range(1, 2 * YS)]
    for friend in friends:
        pl.semaphore_signal(barrier, inc=1, device_id=friend, device_id_type=pl.DeviceIdType.MESH)
    for j in (0, 8, 7, 1, 6, 2, 3, 4, 5):
        loads[j].start()

    slot = lax.broadcasted_iota(jnp.int32, (XS, 1), 0)
    owner = (lax.rem(x + slot, XS) * ZL + zl).astype(F32)
    before = (lax.broadcasted_iota(jnp.int32, (toks, toks), 0)
              < lax.broadcasted_iota(jnp.int32, (toks, toks), 1)).astype(F32).astype(BF)
    gi[...] = jnp.zeros_like(gi)
    go[...] = jnp.zeros_like(go)
    loads[7].wait()
    loads[8].wait()
    idg[0, 8:8 + choices] = own[...].astype(F32)
    loads[0].wait()
    row_id = lax.broadcasted_iota(jnp.int32, (CAP, toks), 0).astype(F32)
    row_all = lax.broadcasted_iota(jnp.int32, (toks, toks), 0).astype(F32)
    lane_id = lax.broadcasted_iota(jnp.int32, (toks, ROWS), 1).astype(F32)

    def route(i):
        gate = jnp.zeros((XS, toks), F32)
        hits = jnp.zeros((XS, toks), F32)
        for c in range(choices):
            hit = idg[i, 8 + c:9 + c] == owner
            gate += jnp.where(hit, idg[i, c:c + 1], 0.0)
            hits += hit.astype(F32)
        m = jnp.concatenate([gate, jnp.where(hits > 0.0, mm(hits.astype(BF), before), VOID)], axis=0)
        mbuf[i] = m
        return m

    def picks(i):
        m = route(i)
        return jnp.concatenate(
            [(row_id == m[XS + q:XS + q + 1]).astype(F32) for q in range(XS)], axis=0).astype(BF)

    def compact(i, hot):
        rows = mm(hot, tbuf[i]).astype(BF)
        srecv[i, 0:CAP] = rows[0:CAP]
        ssend[i, CAP:ROWS] = rows[CAP:ROWS]

    def spread(i):
        for q in range(1, XS):
            x_copy(i, q).start()

    def expert(i):
        group(three(srecv, i, CAP), x_r.at[i]).wait_recv()
        rows = srecv[i]
        g = mm_nt(rows, wg[...])
        u = mm_nt(rows, wu[...])
        h = (g / (1.0 + jnp.exp(-g)) * u).astype(BF)
        hbuf[i] = h
        adm = ad[...]
        low = mm_nt(h, adm).astype(BF)
        p, lanes = i // 2, slice(i % 2 * CAP, (i % 2 + 1) * CAP)
        for q in range(XS):
            t = mm_nt(adm, h[q * CAP:(q + 1) * CAP]).astype(BF)
            if q == 0:
                lrr[p, 0:depth, lanes] = t
            else:
                lrs[p, q * depth:(q + 1) * depth, lanes] = t
        out = (mm(h, wd[...]) + mm(low, abuf[0:depth])).astype(BF)
        oret[i, 0:CAP] = out[0:CAP]
        osend[i, CAP:ROWS] = out[CAP:ROWS]
        if i % 2 == 1:
            for q in range(1, XS):
                lr_copy(p, q).start()

    def grad_in(t):
        group(three(lgr, t, depth), lg_r.at[t]).wait_recv()
        acc = gi[:, 0:hidden]
        for n in range(8):
            if TILE[n] != t:
                continue
            lanes = slice(SIDE[n] * CAP, (SIDE[n] + 1) * CAP)
            for q in range(XS):
                acc += mm(lgr[t, q * depth:(q + 1) * depth, lanes], hbuf[n, q * CAP:(q + 1) * CAP])
        gi[:, 0:hidden] = acc

    seen_low = []
    seen_tile = []

    def grads(n):
        t, p = TILE[n], n // 2
        rows = slice(SIDE[n] * CAP, (SIDE[n] + 1) * CAP)
        lanes = slice(n % 2 * CAP, (n % 2 + 1) * CAP)
        if p not in seen_low:
            seen_low.append(p)
            group(three(lrr, p, depth), lr_r.at[p]).wait_recv()
        m = mbuf[n]
        dy = dbuf[n]
        base = mm_nt(abuf[...], dy)
        lows = []
        packs = []
        for q in range(XS):
            gate = m[q:q + 1]
            rank = m[XS + q:XS + q + 1]
            lg = (base[q * depth:(q + 1) * depth] * gate).astype(BF)
            hot = (row_all == rank + float(SIDE[n] * CAP)).astype(F32).astype(BF)
            packs.append(mm_nt(lg, hot))
            low = mm(lrr[p, q * depth:(q + 1) * depth, lanes], hot[rows])
            lows.append((low * gate).astype(BF))
        pack = jnp.concatenate(packs, axis=0)
        if t in seen_tile:
            pack += lgs[t].astype(F32)
        lgs[t] = pack.astype(BF)
        last = t in seen_tile or TILE.count(t) == 1
        seen_tile.append(t)
        if last:
            for q in range(1, XS):
                lg_copy(t, q).start()
            lgr[t, 0:depth] = pack[0:depth].astype(BF)
        go[...] += mm(jnp.concatenate(lows, axis=0), dy)

    def dy_in(i):
        dy_copy(i).wait_recv()
        if i <= 4:
            dy_copy(i + 2).start()
        if i == 3:
            dy_copy(7).start()

    def pass_on(i, h):
        if h == 0:
            m_copy(i).start()
        tok_copy(i, h).start()

    def tokens_in(i):
        m_copy(i).wait_recv()
        hot = picks(i)
        for h in (0, 1):
            tok_copy(i, h).wait_recv()
            if 1 < i <= 5:
                pass_on(i + 2, h)
        compact(i, hot)
        spread(i)
        if i == 1:
            pass_on(3, 0)
            pass_on(3, 1)

    def returns(i):
        for q in range(1, XS):
            o_copy(i, q).start()

    compact(0, picks(0))
    pl.semaphore_wait(barrier, len(friends))

    m_copy(1).start()
    for h in (0, 1):
        tok_copy(1, h).start()
    spread(0)
    group(tbuf.at[0, pl.ds(0, lead)], t_s.at[0]).wait_send()
    m_copy(2).start()
    for h in (0, 1):
        tok_copy(2, h).start()
    for j in (1, 6, 2, 3, 4, 5):
        loads[j].wait()
    for q in range(1, XS):
        a_copy(q).start()
    tokens_in(1)
    expert(0)
    tokens_in(2)
    tokens_in(3)
    dy_copy(1).start()
    expert(1)
    tokens_in(4)
    dy_copy(2).start()
    expert(2)
    tokens_in(5)
    expert(3)
    tokens_in(6)
    group(abuf.at[pl.ds(depth, 3 * depth)], a_r).wait_recv()
    grads(0)
    expert(4)
    dy_in(2)
    dy_in(1)
    tokens_in(7)
    pl.semaphore_signal(far, inc=1, device_id=at(x, ring(-4 * way)), device_id_type=pl.DeviceIdType.MESH)
    grads(1)
    grads(2)
    expert(5)
    expert(6)
    returns(6)
    dy_in(4)
    dy_in(3)
    expert(7)
    returns(7)
    returns(5)
    grads(4)
    grads(3)
    dy_in(6)
    grads(6)
    dy_in(5)
    grads(5)
    dy_in(7)
    grads(7)
    for j in range(2 * YS):
        goc[j] = go[:, j * 128:(j + 1) * 128]
    for r in range(1, 2 * YS):
        gy_copy(r).start()
    returns(4)

    def combine(i):
        mt = mbuf[i].T
        wt = jnp.zeros((toks, ROWS), F32)
        for q in range(XS):
            wt = jnp.where(lane_id == mt[:, XS + q:XS + q + 1] + float(q * CAP), mt[:, q:q + 1], wt)
        hi = wt.astype(BF)
        lo = (wt - hi.astype(F32)).astype(BF)
        group(three(oret, i, CAP), o_r.at[i]).wait_recv()
        rows = oret[i]
        for h in (0, 1):
            keep = slice(h * half, (h + 1) * half)
            both = mm(jnp.concatenate([hi[keep], lo[keep]], axis=0), rows)
            part = both[0:half] + both[half:]
            if i == 0:
                for j in (1, 2):
                    rs_copy(j, h).wait_recv()
                    part += rsr[j, keep].astype(F32)
                mixed_ref[keep] = part.astype(BF)
                continue
            if i < 6:
                rs_copy(i + 2, h).wait_recv()
                part += rsr[i + 2, keep].astype(F32)
            rss[i, keep] = part.astype(BF)
            rs_copy(i, h).start()

    def sum_a():
        for j in range(2 * YS):
            if j * 128 < hidden:
                dpa[j] = gi[:, j * 128:(j + 1) * 128]
            else:
                dpa[j] = jnp.zeros((depth, 128), F32)
        for r in range(1, 2 * YS):
            da_copy(r).start()

    def sum_x():
        group(goy.at[pl.ds(1, 2 * YS - 1)], gy_r).wait_recv()
        mine = goc[k]
        for r in range(1, 2 * YS):
            mine += goy[r]
        gox[...] = mine
        for q in range(1, XS):
            go_copy(q).start()

    def sum_b():
        group(dpr.at[pl.ds(1, 2 * YS - 1)], da_r).wait_recv()
        mine = dpa[k]
        for r in range(1, 2 * YS):
            mine += dpr[r]
        dpb[depth:2 * depth] = mine
        group(gor.at[pl.ds(depth, 3 * depth)], go_r).wait_recv()
        mine = gox[0:depth]
        for q in range(1, XS):
            mine += gor[q * depth:(q + 1) * depth]
        dpb[0:depth] = mine
        pl.semaphore_wait(far, 1)
        db_copy().start()

    def sum_c():
        db_copy().wait_recv()
        fin = (dpb[...] + dpq[...]).astype(BF)
        dpo[...] = fin
        dpf[0] = fin
        for r in range(1, 2 * YS):
            dc_copy(r).start()

    combine(7)
    grad_in(0)
    grad_in(1)
    combine(6)
    returns(3)
    grad_in(2)
    grad_in(3)
    grad_in(4)
    sum_a()
    sum_x()
    combine(5)
    returns(2)
    sum_b()
    combine(4)
    returns(1)
    combine(3)
    returns(0)
    combine(2)
    sum_c()
    combine(1)
    combine(0)
    group(dpf.at[pl.ds(1, 2 * YS - 1)], dc_r).wait_recv()
    for j in range(2 * YS):
        piece = dpf[lax.rem(k - j + 2 * YS, 2 * YS)]
        gout_ref[:, j * 128:(j + 1) * 128] = piece[0:depth]
        width = min(128, hidden - j * 128)
        if width > 0:
            gin_ref[:, j * 128:j * 128 + width] = piece[depth:2 * depth, 0:width]

    seven = pl.ds(1, 7)
    group(tbuf.at[0, pl.ds(lead, toks - lead)], t_s.at[1]).wait_send()
    group(tbuf.at[pl.ds(2, 6)], t_s.at[2]).wait_send()
    group(idg.at[seven], m_s).wait_send()
    group(dbuf.at[seven], d_s).wait_send()
    group(rss.at[seven], r_s).wait_send()
    group(abuf.at[pl.ds(depth, 3 * depth)], a_s).wait_send()
    group(gox.at[pl.ds(depth, 3 * depth)], go_s).wait_send()
    group(goy.at[seven], gy_s).wait_send()
    group(ssend.at[:, pl.ds(CAP, 3 * CAP)], x_s).wait_send()
    group(osend.at[:, pl.ds(CAP, 3 * CAP)], o_s).wait_send()
    group(lgs.at[:, pl.ds(depth, 3 * depth)], lg_s).wait_send()
    group(lrs.at[:, pl.ds(depth, 3 * depth)], lr_s).wait_send()
    group(dpr.at[seven], da_s).wait_send()
    group(dpf.at[seven], dc_s).wait_send()
    db_copy().wait_send()


def settle(a_ref, b_ref, c_ref, ao_ref, bo_ref, co_ref):
    ao_ref[...] = a_ref[...]
    bo_ref[0] = b_ref[...]
    co_ref[0] = c_ref[...]


def shards(tokens, ids, gates, dy, wg, wu, wd, ad, au):
    toks, width = tokens.shape
    depth, hidden = ad.shape[1], ad.shape[2]
    hbm = pl.BlockSpec(memory_space=pltpu.HBM)
    vmem = pl.BlockSpec(memory_space=pltpu.VMEM)
    dma = pltpu.SemaphoreType.DMA
    V = pltpu.VMEM
    mixed, gin, gout = pl.pallas_call(
        kernel,
        name="moe",
        out_shape=(
            jax.ShapeDtypeStruct((toks, width), BF),
            jax.ShapeDtypeStruct((depth, hidden), BF),
            jax.ShapeDtypeStruct((depth, width), BF),
        ),
        in_specs=[hbm] * 9,
        out_specs=(vmem, vmem, vmem),
        scratch_shapes=[
            V((8, toks, width), BF), V((8, toks, width), BF), V(ids.shape[::-1], ids.dtype), V((8, 16, toks), F32),
            V((8, 2 * XS, toks), F32),
            V((XS * depth, width), BF),
            V((hidden, width), BF), V((hidden, width), BF), V((hidden, width), BF), V((depth, hidden), BF),
            V((8, ROWS, width), BF), V((8, ROWS, width), BF), V((8, ROWS, hidden), BF),
            V((8, ROWS, width), BF), V((8, ROWS, width), BF),
            V((5, XS * depth, 128), BF), V((5, XS * depth, 128), BF),
            V((4, XS * depth, 128), BF), V((4, XS * depth, 128), BF),
            V((8, toks, width), BF), V((8, toks, width), BF),
            V((depth, 768), F32), V((XS * depth, width), F32), V((8, XS * depth, 128), F32), V((8, XS * depth, 128), F32),
            V((XS * depth, 128), F32), V((XS * depth, 128), F32),
            V((8, depth, 128), F32), V((8, depth, 128), F32),
            V((2 * depth, 128), F32), V((2 * depth, 128), F32), V((2 * depth, 128), BF),
            V((8, 2 * depth, 128), BF),
            dma((9,)), dma((3,)), dma((8, 2)), dma(()), dma((8,)), dma(()), dma((8,)), dma(()), dma(()),
            dma(()), dma((8,)), dma(()), dma((8,)), dma(()), dma((8,)), dma(()), dma((8,)),
            dma(()), dma((8, 2)), dma(()), dma(()), dma(()), dma(()), dma(()), dma(()), dma(()), dma(()), dma(()), dma(()),
            pltpu.SemaphoreType.REGULAR,
        ],
        compiler_params=pltpu.CompilerParams(
            collective_id=0, has_side_effects=True, vmem_limit_bytes=48 * 1024 * 1024),
    )(*(pltpu.with_memory_space_constraint(v, pltpu.HBM) for v in (
        ids.T, gates.T, tokens, dy, wg.swapaxes(1, 2), wu.swapaxes(1, 2), wd, ad, au)))
    mixed, gin, gout = pl.pallas_call(
        settle,
        name="settle",
        out_shape=(
            jax.ShapeDtypeStruct((toks, width), BF),
            jax.ShapeDtypeStruct((1, depth, hidden), BF),
            jax.ShapeDtypeStruct((1, depth, width), BF),
        ),
        in_specs=[vmem] * 3,
        out_specs=(vmem, vmem, vmem),
        compiler_params=pltpu.CompilerParams(vmem_limit_bytes=4 * 1024 * 1024),
    )(mixed, gin, gout)
    return mixed, gin, gout


def solution(mesh):
    tok = P(("dp", "expert"), None)
    exp = P("expert", None, None)
    return jax.shard_map(
        shards,
        mesh=mesh,
        in_specs=(tok, tok, tok, tok, exp, exp, exp, exp, exp),
        out_specs=(tok, exp, exp),
        check_vma=False,
    )
```

```python
import functools

import jax
import jax.numpy as jnp
from jax import lax
from jax.experimental import pallas as pl
from jax.experimental.pallas import tpu as pltpu
from jax.sharding import PartitionSpec as P

BF = jnp.bfloat16
F32 = jnp.float32
XS, ZL, ZS, YS = 4, 8, 16, 4
CAP = 48
ROWS = XS * CAP
VOID = -1000.0
TILE = (0, 1, 1, 2, 2, 3, 3, 4)
SIDE = (0, 0, 1, 1, 0, 1, 0, 0)


def mm(a, b):
    return jnp.dot(a, b, preferred_element_type=F32)


def mm_nt(a, b):
    return lax.dot_general(a, b, (((1,), (1,)), ((), ())), preferred_element_type=F32)


def kernel(
    ids_hbm, gates_hbm, tok_hbm, dy_hbm, wg_hbm, wu_hbm, wd_hbm, ad_hbm, au_hbm,
    mixed_ref, gin_ref, gout_ref,
    tbuf, dbuf, own, idg, mbuf, abuf, wg, wu, wd, ad,
    ssend, srecv, hbuf, osend, oret, lgs, lgr, lrs, lrr, rss, rsr,
    gi, go, gob, gor, dpa, dpr, dpb, dpq, dpo, dpf,
    ld_sem, t_s, t_r, m_s, m_r, d_s, d_r, a_s, a_r, x_s, x_r, lg_s, lg_r,
    o_s, o_r, lr_s, lr_r, r_s, r_r, go_s, go_r, da_s, da_r, db_s, db_r, dc_s, dc_r, far,
):
    depth = ad_hbm.shape[1]
    hidden = wg_hbm.shape[1]
    choices = ids_hbm.shape[0]
    toks = tok_hbm.shape[0]
    half = toks // 2
    lead = toks // 4 * 3
    d = lax.axis_index("dp")
    e = lax.axis_index("expert")
    core = lax.rem(d, 2)
    y = lax.rem(lax.div(d, 2), YS)
    zh = lax.div(d, 2 * YS)
    x = lax.div(e, ZL)
    zl = lax.rem(e, ZL)
    z = zh * ZL + zl
    way = 1 - 2 * core
    k = y * 2 + core

    def at(x_, z_):
        return {"dp": lax.div(z_, ZL) * (2 * YS) + k, "expert": x_ * ZL + lax.rem(z_, ZL)}

    def ring(step):
        return lax.rem(z + step + ZS, ZS)

    def xq(q):
        return lax.rem(x + q + XS, XS)

    def peer(r):
        kk = lax.rem(k + r, 2 * YS)
        return kk, {"dp": zh * (2 * YS) + kk, "expert": e}

    def remote(src, dst, s, r, dev):
        return pltpu.make_async_remote_copy(
            src_ref=src, dst_ref=dst, send_sem=s, recv_sem=r,
            device_id=dev, device_id_type=pl.DeviceIdType.MESH)

    def group(ref, s):
        return remote(ref, ref, s, s, at(x, z))

    def three(ref, i, size):
        return ref.at[i, pl.ds(size, 3 * size)]

    def out_step(i):
        return way * (2 * lax.rem(i, 2) - 1)

    def tok_copy(i, h):
        src = max(i - 2, 0)
        rows = pl.ds(h * half, half)
        if i == 1:
            rows = pl.ds(h * lead, toks - lead if h else lead)
        return remote(tbuf.at[src, rows], tbuf.at[i, rows], t_s.at[h if i == 1 else 2], t_r.at[i, h],
                      at(x, ring(out_step(i))))

    def dy_copy(i):
        hops = 2 if i == 7 else 1
        return remote(dbuf.at[max(i - 2 * hops, 0)], dbuf.at[i], d_s, d_r.at[i],
                      at(x, ring(out_step(i) * hops)))

    def m_copy(i):
        src = jnp.maximum(i - 2, 0)
        return remote(idg.at[src], idg.at[i], m_s, m_r.at[i], at(x, ring(out_step(i))))

    def a_copy(q):
        return remote(abuf.at[pl.ds(0, depth)], abuf.at[pl.ds(q * depth, depth)],
                      a_s, a_r, at(xq(-q), z))

    def x_copy(i, q):
        rows = pl.ds(q * CAP, CAP)
        return remote(ssend.at[i, rows], srecv.at[i, rows], x_s, x_r.at[i], at(xq(q), z))

    def lg_copy(i, q):
        rows = pl.ds(q * depth, depth)
        return remote(lgs.at[i, rows], lgr.at[i, rows], lg_s, lg_r.at[i], at(xq(q), z))

    def o_copy(i, q):
        rows = pl.ds(q * CAP, CAP)
        return remote(osend.at[i, rows], oret.at[i, rows], o_s, o_r.at[i], at(xq(-q), z))

    def lr_copy(i, q):
        rows = pl.ds(q * depth, depth)
        return remote(lrs.at[i, rows], lrr.at[i, rows], lr_s, lr_r.at[i], at(xq(-q), z))

    def rs_copy(i, h):
        rows = pl.ds(h * half, half)
        return remote(rss.at[i, rows], rsr.at[i, rows], r_s, r_r.at[i, h],
                      at(x, ring(-out_step(i))))

    def go_copy(q):
        return remote(gob.at[pl.ds(q * depth, depth)], gor.at[pl.ds(q * depth, depth)],
                      go_s, go_r, at(xq(q), z))

    def da_copy(r):
        kk, dev = peer(r)
        return remote(dpa.at[kk], dpr.at[r], da_s, da_r, dev)

    def db_copy():
        return remote(dpb, dpq, db_s, db_r, at(x, ring(ZL)))

    def dc_copy(r):
        _, dev = peer(r)
        return remote(dpo, dpf.at[r], dc_s, dc_r, dev)

    loads = [
        pltpu.make_async_copy(tok_hbm, tbuf.at[0], ld_sem.at[0]),
        pltpu.make_async_copy(au_hbm.at[0], abuf.at[pl.ds(0, depth)], ld_sem.at[1]),
        pltpu.make_async_copy(wg_hbm.at[0], wg, ld_sem.at[2]),
        pltpu.make_async_copy(wu_hbm.at[0], wu, ld_sem.at[3]),
        pltpu.make_async_copy(wd_hbm.at[0], wd, ld_sem.at[4]),
        pltpu.make_async_copy(ad_hbm.at[0], ad, ld_sem.at[5]),
        pltpu.make_async_copy(dy_hbm, dbuf.at[0], ld_sem.at[6]),
        pltpu.make_async_copy(ids_hbm, own, ld_sem.at[7]),
        pltpu.make_async_copy(gates_hbm, idg.at[0, pl.ds(0, choices)], ld_sem.at[8]),
    ]
    barrier = pltpu.get_barrier_semaphore()
    friends = [at(x, ring(s)) for s in (1, -1)]
    friends += [at(xq(q), z) for q in range(1, XS)]
    friends += [peer(r)[1] for r in range(1, 2 * YS)]
    for friend in friends:
        pl.semaphore_signal(barrier, inc=1, device_id=friend, device_id_type=pl.DeviceIdType.MESH)
    for j in (0, 8, 7, 1, 6, 2, 3, 4, 5):
        loads[j].start()

    slot = lax.broadcasted_iota(jnp.int32, (XS, 1), 0)
    owner = (lax.rem(x + slot, XS) * ZL + zl).astype(F32)
    before = (lax.broadcasted_iota(jnp.int32, (toks, toks), 0)
              < lax.broadcasted_iota(jnp.int32, (toks, toks), 1)).astype(F32).astype(BF)
    gi[...] = jnp.zeros_like(gi)
    go[...] = jnp.zeros_like(go)
    loads[7].wait()
    loads[8].wait()
    idg[0, 8:8 + choices] = own[...].astype(F32)
    loads[0].wait()
    row_id = lax.broadcasted_iota(jnp.int32, (CAP, toks), 0).astype(F32)
    row_all = lax.broadcasted_iota(jnp.int32, (toks, toks), 0).astype(F32)
    lane_id = lax.broadcasted_iota(jnp.int32, (toks, ROWS), 1).astype(F32)

    def route(i):
        gate = jnp.zeros((XS, toks), F32)
        hits = jnp.zeros((XS, toks), F32)
        for c in range(choices):
            hit = idg[i, 8 + c:9 + c] == owner
            gate += jnp.where(hit, idg[i, c:c + 1], 0.0)
            hits += hit.astype(F32)
        m = jnp.concatenate([gate, jnp.where(hits > 0.0, mm(hits.astype(BF), before), VOID)], axis=0)
        mbuf[i] = m
        return m

    def picks(i):
        m = route(i)
        return jnp.concatenate(
            [(row_id == m[XS + q:XS + q + 1]).astype(F32) for q in range(XS)], axis=0).astype(BF)

    def compact(i, hot):
        rows = mm(hot, tbuf[i]).astype(BF)
        srecv[i, 0:CAP] = rows[0:CAP]
        ssend[i, CAP:ROWS] = rows[CAP:ROWS]

    def spread(i):
        for q in range(1, XS):
            x_copy(i, q).start()

    def expert(i):
        group(three(srecv, i, CAP), x_r.at[i]).wait_recv()
        rows = srecv[i]
        g = mm_nt(rows, wg[...])
        u = mm_nt(rows, wu[...])
        h = (g / (1.0 + jnp.exp(-g)) * u).astype(BF)
        hbuf[i] = h
        adm = ad[...]
        low = mm_nt(h, adm).astype(BF)
        p, lanes = i // 2, slice(i % 2 * CAP, (i % 2 + 1) * CAP)
        for q in range(XS):
            t = mm_nt(adm, h[q * CAP:(q + 1) * CAP]).astype(BF)
            if q == 0:
                lrr[p, 0:depth, lanes] = t
            else:
                lrs[p, q * depth:(q + 1) * depth, lanes] = t
        out = (mm(h, wd[...]) + mm(low, abuf[0:depth])).astype(BF)
        oret[i, 0:CAP] = out[0:CAP]
        osend[i, CAP:ROWS] = out[CAP:ROWS]
        if i % 2 == 1:
            for q in range(1, XS):
                lr_copy(p, q).start()

    def grad_in(t):
        group(three(lgr, t, depth), lg_r.at[t]).wait_recv()
        acc = gi[:, 0:hidden]
        for n in range(8):
            if TILE[n] != t:
                continue
            lanes = slice(SIDE[n] * CAP, (SIDE[n] + 1) * CAP)
            for q in range(XS):
                acc += mm(lgr[t, q * depth:(q + 1) * depth, lanes], hbuf[n, q * CAP:(q + 1) * CAP])
        gi[:, 0:hidden] = acc

    seen_low = []
    seen_tile = []

    def grads(n):
        t, p = TILE[n], n // 2
        rows = slice(SIDE[n] * CAP, (SIDE[n] + 1) * CAP)
        lanes = slice(n % 2 * CAP, (n % 2 + 1) * CAP)
        if p not in seen_low:
            seen_low.append(p)
            group(three(lrr, p, depth), lr_r.at[p]).wait_recv()
        m = mbuf[n]
        dy = dbuf[n]
        base = mm_nt(abuf[...], dy)
        lows = []
        packs = []
        for q in range(XS):
            gate = m[q:q + 1]
            rank = m[XS + q:XS + q + 1]
            lg = (base[q * depth:(q + 1) * depth] * gate).astype(BF)
            hot = (row_all == rank + float(SIDE[n] * CAP)).astype(F32).astype(BF)
            packs.append(mm_nt(lg, hot))
            low = mm(lrr[p, q * depth:(q + 1) * depth, lanes], hot[rows])
            lows.append((low * gate).astype(BF))
        pack = jnp.concatenate(packs, axis=0)
        if t in seen_tile:
            pack += lgs[t].astype(F32)
        lgs[t] = pack.astype(BF)
        last = t in seen_tile or TILE.count(t) == 1
        seen_tile.append(t)
        if last:
            for q in range(1, XS):
                lg_copy(t, q).start()
            lgr[t, 0:depth] = pack[0:depth].astype(BF)
        go[...] += mm(jnp.concatenate(lows, axis=0), dy)

    def dy_in(i):
        dy_copy(i).wait_recv()
        if i <= 4:
            dy_copy(i + 2).start()
        if i == 3:
            dy_copy(7).start()

    def pass_on(i, h):
        if h == 0:
            m_copy(i).start()
        tok_copy(i, h).start()

    def tokens_in(i):
        m_copy(i).wait_recv()
        hot = picks(i)
        for h in (0, 1):
            tok_copy(i, h).wait_recv()
            if 1 < i <= 5:
                pass_on(i + 2, h)
        compact(i, hot)
        spread(i)
        if i == 1:
            pass_on(3, 0)
            pass_on(3, 1)

    def returns(i):
        for q in range(1, XS):
            o_copy(i, q).start()

    compact(0, picks(0))
    pl.semaphore_wait(barrier, len(friends))

    m_copy(1).start()
    for h in (0, 1):
        tok_copy(1, h).start()
    spread(0)
    group(tbuf.at[0, pl.ds(0, lead)], t_s.at[0]).wait_send()
    m_copy(2).start()
    for h in (0, 1):
        tok_copy(2, h).start()
    for j in (1, 6, 2, 3, 4, 5):
        loads[j].wait()
    for q in range(1, XS):
        a_copy(q).start()
    tokens_in(1)
    expert(0)
    tokens_in(2)
    tokens_in(3)
    dy_copy(1).start()
    expert(1)
    tokens_in(4)
    dy_copy(2).start()
    expert(2)
    tokens_in(5)
    expert(3)
    tokens_in(6)
    group(abuf.at[pl.ds(depth, 3 * depth)], a_r).wait_recv()
    grads(0)
    expert(4)
    dy_in(2)
    dy_in(1)
    tokens_in(7)
    pl.semaphore_signal(far, inc=1, device_id=at(x, ring(-4 * way)), device_id_type=pl.DeviceIdType.MESH)
    grads(1)
    grads(2)
    expert(5)
    expert(6)
    returns(6)
    dy_in(4)
    dy_in(3)
    expert(7)
    returns(7)
    returns(5)
    grads(4)
    grads(3)
    dy_in(6)
    grads(6)
    dy_in(5)
    grads(5)
    dy_in(7)
    grads(7)
    gob[...] = go[...].astype(BF)
    for q in range(1, XS):
        go_copy(q).start()
    returns(4)

    def combine(i):
        mt = mbuf[i].T
        wt = jnp.zeros((toks, ROWS), F32)
        for q in range(XS):
            wt = jnp.where(lane_id == mt[:, XS + q:XS + q + 1] + float(q * CAP), mt[:, q:q + 1], wt)
        hi = wt.astype(BF)
        lo = (wt - hi.astype(F32)).astype(BF)
        group(three(oret, i, CAP), o_r.at[i]).wait_recv()
        rows = oret[i]
        for h in (0, 1):
            keep = slice(h * half, (h + 1) * half)
            both = mm(jnp.concatenate([hi[keep], lo[keep]], axis=0), rows)
            part = both[0:half] + both[half:]
            if i == 0:
                for j in (1, 2):
                    rs_copy(j, h).wait_recv()
                    part += rsr[j, keep].astype(F32)
                mixed_ref[keep] = part.astype(BF)
                continue
            if i < 6:
                rs_copy(i + 2, h).wait_recv()
                part += rsr[i + 2, keep].astype(F32)
            rss[i, keep] = part.astype(BF)
            rs_copy(i, h).start()

    def sum_a():
        group(gor.at[pl.ds(depth, 3 * depth)], go_r).wait_recv()
        total = go[0:depth]
        for q in range(1, XS):
            total += gor[q * depth:(q + 1) * depth].astype(F32)
        for j in range(2 * YS):
            cols = slice(j * 128, (j + 1) * 128)
            dpa[j, 0:depth] = total[:, cols]
            if j * 128 < hidden:
                dpa[j, depth:2 * depth] = gi[:, cols]
            else:
                dpa[j, depth:2 * depth] = jnp.zeros((depth, 128), F32)
        for r in range(1, 2 * YS):
            da_copy(r).start()

    def sum_b():
        mine = dpa[k]
        group(dpr.at[pl.ds(1, 2 * YS - 1)], da_r).wait_recv()
        for r in range(1, 2 * YS):
            mine += dpr[r]
        dpb[...] = mine
        pl.semaphore_wait(far, 1)
        db_copy().start()

    def sum_c():
        db_copy().wait_recv()
        fin = (dpb[...] + dpq[...]).astype(BF)
        dpo[...] = fin
        dpf[0] = fin
        for r in range(1, 2 * YS):
            dc_copy(r).start()

    combine(7)
    grad_in(0)
    grad_in(1)
    combine(6)
    returns(3)
    grad_in(2)
    grad_in(3)
    grad_in(4)
    sum_a()
    combine(5)
    returns(2)
    sum_b()
    combine(4)
    returns(1)
    combine(3)
    returns(0)
    combine(2)
    sum_c()
    combine(1)
    combine(0)
    group(dpf.at[pl.ds(1, 2 * YS - 1)], dc_r).wait_recv()
    for j in range(2 * YS):
        piece = dpf[lax.rem(k - j + 2 * YS, 2 * YS)]
        gout_ref[:, j * 128:(j + 1) * 128] = piece[0:depth]
        width = min(128, hidden - j * 128)
        if width > 0:
            gin_ref[:, j * 128:j * 128 + width] = piece[depth:2 * depth, 0:width]

    seven = pl.ds(1, 7)
    group(tbuf.at[0, pl.ds(lead, toks - lead)], t_s.at[1]).wait_send()
    group(tbuf.at[pl.ds(2, 6)], t_s.at[2]).wait_send()
    group(idg.at[seven], m_s).wait_send()
    group(dbuf.at[seven], d_s).wait_send()
    group(rss.at[seven], r_s).wait_send()
    group(abuf.at[pl.ds(depth, 3 * depth)], a_s).wait_send()
    group(gob.at[pl.ds(depth, 3 * depth)], go_s).wait_send()
    group(ssend.at[:, pl.ds(CAP, 3 * CAP)], x_s).wait_send()
    group(osend.at[:, pl.ds(CAP, 3 * CAP)], o_s).wait_send()
    group(lgs.at[:, pl.ds(depth, 3 * depth)], lg_s).wait_send()
    group(lrs.at[:, pl.ds(depth, 3 * depth)], lr_s).wait_send()
    group(dpr.at[seven], da_s).wait_send()
    group(dpf.at[seven], dc_s).wait_send()
    db_copy().wait_send()


def settle(a_ref, b_ref, c_ref, ao_ref, bo_ref, co_ref):
    ao_ref[...] = a_ref[...]
    bo_ref[0] = b_ref[...]
    co_ref[0] = c_ref[...]


def shards(tokens, ids, gates, dy, wg, wu, wd, ad, au):
    toks, width = tokens.shape
    depth, hidden = ad.shape[1], ad.shape[2]
    hbm = pl.BlockSpec(memory_space=pltpu.HBM)
    vmem = pl.BlockSpec(memory_space=pltpu.VMEM)
    dma = pltpu.SemaphoreType.DMA
    V = pltpu.VMEM
    mixed, gin, gout = pl.pallas_call(
        kernel,
        name="moe",
        out_shape=(
            jax.ShapeDtypeStruct((toks, width), BF),
            jax.ShapeDtypeStruct((depth, hidden), BF),
            jax.ShapeDtypeStruct((depth, width), BF),
        ),
        in_specs=[hbm] * 9,
        out_specs=(vmem, vmem, vmem),
        scratch_shapes=[
            V((8, toks, width), BF), V((8, toks, width), BF), V(ids.shape[::-1], ids.dtype), V((8, 16, toks), F32),
            V((8, 2 * XS, toks), F32),
            V((XS * depth, width), BF),
            V((hidden, width), BF), V((hidden, width), BF), V((hidden, width), BF), V((depth, hidden), BF),
            V((8, ROWS, width), BF), V((8, ROWS, width), BF), V((8, ROWS, hidden), BF),
            V((8, ROWS, width), BF), V((8, ROWS, width), BF),
            V((5, XS * depth, 128), BF), V((5, XS * depth, 128), BF),
            V((4, XS * depth, 128), BF), V((4, XS * depth, 128), BF),
            V((8, toks, width), BF), V((8, toks, width), BF),
            V((depth, 768), F32), V((XS * depth, width), F32), V((XS * depth, width), BF), V((XS * depth, width), BF),
            V((8, 2 * depth, 128), F32), V((8, 2 * depth, 128), F32),
            V((2 * depth, 128), F32), V((2 * depth, 128), F32), V((2 * depth, 128), BF),
            V((8, 2 * depth, 128), BF),
            dma((9,)), dma((3,)), dma((8, 2)), dma(()), dma((8,)), dma(()), dma((8,)), dma(()), dma(()),
            dma(()), dma((8,)), dma(()), dma((8,)), dma(()), dma((8,)), dma(()), dma((8,)),
            dma(()), dma((8, 2)), dma(()), dma(()), dma(()), dma(()), dma(()), dma(()), dma(()), dma(()),
            pltpu.SemaphoreType.REGULAR,
        ],
        compiler_params=pltpu.CompilerParams(
            collective_id=0, has_side_effects=True, vmem_limit_bytes=48 * 1024 * 1024),
    )(*(pltpu.with_memory_space_constraint(v, pltpu.HBM) for v in (
        ids.T, gates.T, tokens, dy, wg.swapaxes(1, 2), wu.swapaxes(1, 2), wd, ad, au)))
    mixed, gin, gout = pl.pallas_call(
        settle,
        name="settle",
        out_shape=(
            jax.ShapeDtypeStruct((toks, width), BF),
            jax.ShapeDtypeStruct((1, depth, hidden), BF),
            jax.ShapeDtypeStruct((1, depth, width), BF),
        ),
        in_specs=[vmem] * 3,
        out_specs=(vmem, vmem, vmem),
        compiler_params=pltpu.CompilerParams(vmem_limit_bytes=4 * 1024 * 1024),
    )(mixed, gin, gout)
    return mixed, gin, gout


def solution(mesh):
    tok = P(("dp", "expert"), None)
    exp = P("expert", None, None)
    return jax.shard_map(
        shards,
        mesh=mesh,
        in_specs=(tok, tok, tok, tok, exp, exp, exp, exp, exp),
        out_specs=(tok, exp, exp),
        check_vma=False,
    )
```
